512 devices in a mesh: win: 16 (over x_hi, y), lat: 32 (over z, x_lo, core).
Axes of the slice: x: 4 (x_hi: 2, x_lo: 2; x = x_hi * 2 + x_lo), y: 8, z: 8, core: 2. Of those that a mesh axis runs over, the one named last changes fastest.
Arguments:
- state: float32 [16, 1, 1024, 2048], P('win', None, 'lat'), may hold values from -6 to 6
- multipliers: float32 [16, 1, 1024, 2048], P('win', None, 'lat'), may hold values from -3 to 3
- observations: float32 [16, 2, 1, 1024, 2048], P('win', None, None, 'lat'), may hold values from -6 to 6
- obs_mask: int32 [16, 2, 1024, 2048], P('win', None, 'lat'), may hold values 0 or 1
- speed: float32 [1], replicated, may hold values from 0.1 to 0.3
- drift: float32 [1], replicated, may hold values from 0.1 to 0.4
- kappa: float32 [1], replicated, may hold values from 0.05 to 0.2
- lat_spectrum: float32 [1, 1024], replicated, may hold values from 0.05 to 1
- lon_spectrum: float32 [1, 2048], replicated, may hold values from 0.05 to 1
Outputs:
- new_state: float32 [16, 1, 1024, 2048], P('win', None, 'lat')
- new_multipliers: float32 [16, 1, 1024, 2048], P('win', None, 'lat')
The draws below stay inside these ranges and needn't reach their ends.
All inputs are finite; a program needn't handle non-finite values. No bound on the sum of `obs_mask` on one device may be relied on, other than what follows from the above.
Results may differ from the reference program's by a relative error of at most 0.0001.
Values sent between devices are 32-bit elements; how exact they have to be, the bound alone decides.
A program may use at most 64 MiB of HBM per device.

```python
import math
import jax
import jax.numpy as jnp
from jax import lax

NLON = 2048
NLAT = 1024
LEV = 1
STEPS = 2
ITERS = 1
NWIN = 16


def place_ends(drawn, rng, smallest, top_value):
    shape = drawn.shape
    index_at = [jax.random.randint(jax.random.fold_in(rng, axis), (), 0, shape[axis]) for axis in range(len(shape))]
    drawn = drawn.at[tuple(index_at)].set(smallest)
    longest = shape.index(max(shape))
    index_at[longest] = (index_at[longest] + 1) % shape[longest]
    return drawn.at[tuple(index_at)].set(top_value)


def levels(own_key, dims, split, least, high):
    loudness = 1.0
    for axis_at, parts in split:
        draws = jax.random.uniform(jax.random.fold_in(jax.random.fold_in(own_key, 6), axis_at), (parts,), jnp.float32, least / len(split), high / len(split))
        loudness = loudness * jnp.repeat(jnp.exp(draws), dims[axis_at] // parts).reshape((-1,) + (1,) * (len(dims) - 1 - axis_at))
    return loudness


def bell_draw(own_key, extent, deviation, limit, pieces=(), held_as=jnp.bfloat16):
    values = jax.random.normal(own_key, extent, jnp.float32) * deviation
    if len(pieces) > 0:
        values = levels(own_key, extent, pieces, -0.22, 0.18) * values
    return jnp.clip(values, min=-limit, max=limit).astype(held_as)


def setup_inputs(seed: int = 0) -> dict:
    arg_keys = jax.random.split(jax.random.key(seed), 10)
    state = bell_draw(arg_keys[0], (NWIN, LEV, NLAT, NLON), 1.0, 6.0, ((0, 16), (2, 32)), jnp.float32)
    multipliers = bell_draw(arg_keys[1], (NWIN, LEV, NLAT, NLON), 0.5, 3.0, ((0, 16), (2, 32)), jnp.float32)
    observations = bell_draw(arg_keys[2], (NWIN, STEPS, LEV, NLAT, NLON), 1.0, 6.0, ((0, 16), (3, 32)), jnp.float32)
    obs_mask = place_ends((jax.random.randint(arg_keys[3], (NWIN, STEPS, NLAT, NLON), 0, 3) < 1).astype(jnp.int32), jax.random.fold_in(arg_keys[3], 1), 0, 1)
    speed = jnp.clip(jax.random.uniform(arg_keys[4], (LEV,), jnp.float32, 0.1, 0.3), 0.1, 0.3)
    drift = jnp.clip(jax.random.uniform(arg_keys[5], (LEV,), jnp.float32, 0.1, 0.4), 0.1, 0.4)
    kappa = jnp.clip(jax.random.uniform(arg_keys[6], (LEV,), jnp.float32, 0.05, 0.2), 0.05, 0.2)
    lat_spectrum = jnp.clip(jnp.exp(jax.random.uniform(arg_keys[7], (LEV, NLAT), jnp.float32, math.log(0.05), math.log(1.0))), 0.05, 1.0)
    lon_spectrum = jnp.clip(jnp.exp(jax.random.uniform(arg_keys[8], (LEV, NLON), jnp.float32, math.log(0.05), math.log(1.0))), 0.05, 1.0)
    return {"state": state, "multipliers": multipliers, "observations": observations, "obs_mask": obs_mask, "speed": speed, "drift": drift, "kappa": kappa, "lat_spectrum": lat_spectrum, "lon_spectrum": lon_spectrum}


def hartley(count):
    index = jnp.arange(count, dtype=jnp.int32)
    product = (index[:, None] * index[None, :]) % count
    angle = product.astype(jnp.float32) * (2.0 * math.pi / count)
    return jnp.cos(angle) + jnp.sin(angle)


def advance(field, speed, drift, kappa):
    east = jnp.roll(field, -1, axis=-1)
    west = jnp.roll(field, 1, axis=-1)
    widths = [(0, 0)] * (field.ndim - 2) + [(1, 1), (0, 0)]
    padded = jnp.pad(field, widths)
    north = padded[..., 2:, :]
    south = padded[..., :-2, :]
    speed_c = speed[:, None, None]
    drift_c = drift[:, None, None]
    kappa_c = kappa[:, None, None]
    return (field - speed_c * field * (east - west) * 0.5 - drift_c * (north - south) * 0.5
            + kappa_c * (east + west + north + south - 4.0 * field))


def reference(state, multipliers, observations, obs_mask, speed, drift, kappa, lat_spectrum, lon_spectrum):
    high = lax.Precision.HIGHEST
    h_lon = hartley(NLON)
    h_lat = hartley(NLAT)
    weight = lat_spectrum[:, :, None] * lon_spectrum[:, None, :]
    mask = obs_mask.astype(jnp.float32)

    def covariance(resid):
        spectral = jnp.matmul(resid, h_lon, precision=high)
        spectral = jnp.einsum('ij,ljk->lik', h_lat, spectral, precision=high) * weight
        spectral = jnp.einsum('ij,ljk->lik', h_lat, spectral, precision=high)
        return jnp.matmul(spectral, h_lon, precision=high) / (NLAT * NLON)

    windows = jnp.arange(NWIN, dtype=jnp.int32)[:, None, None, None]
    field = state
    lam = multipliers
    for loop_index in range(ITERS):
        first = advance(field, speed, drift, kappa)
        second = advance(first, speed, drift, kappa)
        defect = (mask[:, 0][:, None] * (observations[:, 0] - first)
                  + mask[:, 1][:, None] * (observations[:, 1] - second))
        prior_end = jnp.concatenate([jnp.zeros_like(second[:1]), second[:-1]], axis=0)
        mismatch = jnp.where(windows > 0, field - prior_end, jnp.float32(0.0))
        lam = lam + 0.5 * mismatch
        summed = jnp.cumsum(lam, axis=0)
        carried = jnp.concatenate([jnp.zeros_like(lam[:1]), summed[:-1]], axis=0)
        resid = defect + lam - carried / jnp.maximum(windows, 1).astype(jnp.float32)
        field = field + 0.5 * lax.map(covariance, resid)
    return field, lam
```

```python
import functools
import math

import jax
import jax.numpy as jnp
import numpy as np
from jax import lax
from jax.experimental import pallas as pl
from jax.experimental.pallas import tpu as pltpu
from jax.sharding import Mesh
from jax.sharding import PartitionSpec as P

AXES = ("win_0", "win_1", "lat_0", "lat_1", "lat_2")
WIN = AXES[:2]
LAT = AXES[2:]
F32 = jnp.float32
BF16 = jnp.bfloat16
AROUND = (4, 5, 3, 6, 2, 7, 1, 0)
TILE_OF = (1, 0, 2, 3)


def rotated(c, s, angle):
    if s is None:
        return c * math.cos(angle), c * math.sin(angle)
    cos, sin = math.cos(angle), math.sin(angle)
    return c * cos - s * sin, c * sin + s * cos


def rfft(xs):
    n = len(xs)
    if n == 2:
        return [(xs[0] + xs[1], None), (xs[0] - xs[1], None)]
    even, odd = rfft(xs[0::2]), rfft(xs[1::2])
    out = [None] * (n // 2 + 1)
    for k in range(n // 4 + 1):
        (ec, es), (oc, os) = even[k], odd[k]
        if k == 0:
            out[0] = (ec + oc, None)
            out[n // 2] = (ec - oc, None)
        elif k == n // 4:
            out[k] = (ec, oc)
        else:
            tc, ts = rotated(oc, os, 2 * math.pi * k / n)
            if es is None:
                out[k] = (ec + tc, ts)
                out[n // 2 - k] = (ec - tc, ts)
            else:
                out[k] = (ec + tc, es + ts)
                out[n // 2 - k] = (ec - tc, ts - es)
    return out


def synth(n, c, s):
    if n == 2:
        return [c[0] + c[1], c[0] - c[1]]
    half, quarter = n // 2, n // 4
    ec, es, oc, os = [], [], [], []
    for k in range(quarter + 1):
        if k == quarter:
            ec.append(c[k])
            es.append(None)
            oc.append(s[k])
            os.append(None)
        elif k == 0:
            ec.append(c[0] + c[half])
            es.append(None)
            oc.append(c[0] - c[half])
            os.append(None)
        else:
            cos, sin = math.cos(2 * math.pi * k / n), math.sin(2 * math.pi * k / n)
            ec.append(c[k] + c[half - k])
            es.append(s[k] - s[half - k])
            dc, ds = c[k] - c[half - k], s[k] + s[half - k]
            oc.append(dc * cos + ds * sin)
            os.append(ds * cos - dc * sin)
    out = [None] * n
    out[0::2] = synth(half, ec, es)
    out[1::2] = synth(half, oc, os)
    return out


def analyse(xs, cos, sin):
    n = len(xs)
    bins = rfft(xs)
    u, v = [], []
    for k in range(n):
        c, s = bins[k] if k <= n // 2 else bins[n - k]
        if k == 0:
            u.append(c)
            v.append(c * 0.0)
        elif s is None:
            u.append(c * cos[k])
            v.append(c * sin[k])
        elif k <= n // 2:
            u.append(c * cos[k] - s * sin[k])
            v.append(c * sin[k] + s * cos[k])
        else:
            u.append(c * cos[k] + s * sin[k])
            v.append(c * sin[k] - s * cos[k])
    return u, v


def synthesise(u, v, cos, sin):
    n = len(u)
    c, s = [u[0]], [None]
    for k in range(1, n):
        c.append(u[k] * cos[k] + v[k] * sin[k])
        s.append(None if k == n // 2 else v[k] * cos[k] - u[k] * sin[k])
    half = n // 2
    fc = [c[0]] + [c[k] + c[n - k] for k in range(1, half)] + [c[half]]
    fs = [None] + [s[k] - s[n - k] for k in range(1, half)] + [None]
    return synth(n, fc, fs)


def twiddle(n1, n2):
    angle = 2 * np.pi * np.arange(n1)[:, None] * np.arange(n2)[None] / (n1 * n2)
    return np.cos(angle), np.sin(angle)


def casmat(n2):
    angle = 2 * np.pi * (np.arange(n2)[:, None] * np.arange(n2)[None] % n2) / n2
    cos, sin = np.cos(angle), np.sin(angle)
    return np.concatenate([cos + sin, cos - sin], 0)


def tables(n1, n2):
    copies = 128 // n2
    cos, sin = (np.tile(t, (1, copies)) for t in twiddle(n1, n2))
    one = casmat(n2)
    eye = np.eye(copies)
    full = np.concatenate([np.kron(eye, one[:n2]), np.kron(eye, one[n2:])], 0)
    return np.concatenate([cos, sin], 0).astype(np.float32), full.astype(np.float32)


def halves(full):
    import ml_dtypes

    hi = full.astype(ml_dtypes.bfloat16)
    lo = (full - hi.astype(np.float32)).astype(ml_dtypes.bfloat16)
    return np.stack([hi, lo])


def dot3(a, hi, lo):
    a_hi = a.astype(BF16)
    a_lo = (a - a_hi.astype(F32)).astype(BF16)
    dot = functools.partial(jnp.dot, preferred_element_type=F32)
    return dot(a_hi, hi) + (dot(a_lo, hi) + dot(a_hi, lo))


def gathered(spec, n1, n2):
    n = n1 * n2
    rows = lax.broadcasted_iota(jnp.int32, (n1, n), 0)
    lanes = lax.broadcasted_iota(jnp.int32, (n1, n), 1)
    own = jnp.where((lanes & (n1 - 1)) == rows, jnp.broadcast_to(spec, (n1, n)), 0.0)
    first = own.astype(BF16)
    rest = own - first.astype(F32)
    second = rest.astype(BF16)
    third = (rest - second.astype(F32)).astype(BF16)
    place = lax.broadcasted_iota(jnp.int32, (n, 128), 0) >> (n1.bit_length() - 1)
    lane = lax.broadcasted_iota(jnp.int32, (n, 128), 1) & (n2 - 1)
    pick = jnp.where(place == lane, 1.0, 0.0).astype(BF16)
    dot = functools.partial(jnp.dot, preferred_element_type=F32)
    return dot(first, pick) + dot(second, pick) + dot(third, pick)


def slot_of(tile, group):
    return (group // 2) * 8 + (group % 2) * 4 + TILE_OF.index(tile)


def kernel(
    state, mult, obs, mask, speed, drift, kappa, lat_spec, lon_spec, tw, wf, wb,
    new_state, new_mult,
    xb, mb, ob, kb, ls, lo, twb, wfb, wbb,
    halo, x1b, x2b, pb, lb, lamb, a_out, a_in, p_out, p_in,
    rb, tb, zb, yb, ob2, vb, uv, lsf, lnf, outb,
    in_sem, out_sem, h_send, h_recv, a_send, a_recv, p_send, p_recv, e_send, e_recv, z_send, z_recv, y_send, y_recv,
):
    xh, y, z, xl, core = (lax.axis_index(a) for a in AXES)
    w = xh * 8 + y
    l = z * 4 + xl * 2 + core
    group = xl * 2 + core

    def at_win(v):
        return (lax.div(v, 8), lax.rem(v, 8), z, xl, core)

    def at_lat(m):
        return (xh, y, lax.div(m, 4), lax.rem(lax.div(m, 2), 2), lax.rem(m, 2))

    loads = [
        pltpu.make_async_copy(src, dst, in_sem.at[i])
        for i, (src, dst) in enumerate(
            [(state, xb), (mult, mb), (obs, ob), (mask, kb), (lat_spec, ls), (lon_spec, lo), (tw, twb), (wf, wfb), (wb, wbb)]
        )
    ]
    for load in loads:
        load.start()

    barrier = pltpu.get_barrier_semaphore()
    for k in range(1, 16):
        pl.semaphore_signal(barrier, inc=1, device_id=at_win(lax.rem(w + k, 16)), device_id_type=pl.DeviceIdType.MESH)
    for k in range(1, 32):
        pl.semaphore_signal(barrier, inc=1, device_id=at_lat(lax.rem(l + k, 32)), device_id_type=pl.DeviceIdType.MESH)

    sends = []

    def send(src, dst, send_sem, recv_sem, device, when=None):
        copy = pltpu.make_async_remote_copy(
            src_ref=src, dst_ref=dst, send_sem=send_sem, recv_sem=recv_sem,
            device_id=device, device_id_type=pl.DeviceIdType.MESH,
        )
        guarded(when, copy.start)
        sends.append((when, copy))

    def guarded(when, act):
        if when is None:
            act()
        else:
            pl.when(when)(act)

    def arrived(dst, recv_sem, send_sem, device, when=None):
        copy = pltpu.make_async_remote_copy(
            src_ref=dst, dst_ref=dst, send_sem=send_sem, recv_sem=recv_sem,
            device_id=device, device_id_type=pl.DeviceIdType.MESH,
        )
        guarded(when, copy.wait_recv)

    sp, dr, ka = speed[0], drift[0], kappa[0]
    row = lax.broadcasted_iota(jnp.int32, (8, 2048), 0)
    later = jnp.where(w > 0, F32(0.5), F32(0.0))
    inv = F32(1.0)
    for k in range(2, 16):
        inv = jnp.where(w == k, F32(1.0 / k), inv)

    def step(mid, north, south):
        east = pltpu.roll(mid, 2047, 1)
        west = pltpu.roll(mid, 1, 1)
        return (
            mid
            - (sp * mid * (east - west)) * 0.5
            - (dr * (north - south)) * 0.5
            + ka * (east + west + north + south - 4.0 * mid)
        )

    def up(t):
        return pltpu.roll(t, 7, 0)

    def down(t):
        return pltpu.roll(t, 1, 0)

    def advanced(before, mid, after):
        u, d = up(mid), down(mid)
        north = u if after is None else jnp.where(row == 7, up(after), u)
        south = d if before is None else jnp.where(row == 0, down(before), d)
        return step(mid, north, south)

    def tile(ref, t):
        return ref[8 * t : 8 * t + 8, :]

    def finish_tile(t, second):
        a = tile(mb, t) + later * tile(xb, t) - 0.5 * second
        for g in range(4):
            a_out[slot_of(t, g)] = a[:, 512 * g : 512 * g + 512]
            x2b[g, 8 * t : 8 * t + 8, :] = second[:, 512 * g : 512 * g + 512]

    def send_a(odd):
        for off in (2, 1, 3, 0):
            yy = 2 * lax.rem(lax.div(y, 2) + off, 4) + odd
            for far in (1, 0):
                owner = lax.rem(xh + far, 2) * 8 + yy
                when = (lax.rem(y, 2) != odd) if (off == 0 and far == 0) else None
                send(a_out.at[owner], a_in.at[w], a_send.at[owner], a_recv.at[w], at_win(owner), when)

    loads[0].wait()
    first = [tile(xb, t) for t in range(4)]
    for t in range(4):
        x1b[8 * t : 8 * t + 8, :] = advanced(
            first[t - 1] if t > 0 else None, first[t], first[t + 1] if t < 3 else None
        )
    loads[1].wait()
    pl.semaphore_wait(barrier, 46)
    north_of, south_of = lax.rem(l + 1, 32), lax.rem(l + 31, 32)
    send(xb.at[24:32, :], halo.at[0], h_send.at[0], h_recv.at[0], at_lat(north_of), l < 31)
    send(xb.at[0:8, :], halo.at[1], h_send.at[1], h_recv.at[1], at_lat(south_of), l > 0)
    for t in (1, 2):
        finish_tile(t, advanced(tile(x1b, t - 1), tile(x1b, t), tile(x1b, t + 1)))
    send_a(0)

    @pl.when(l == 0)
    def _():
        halo[0] = jnp.zeros((8, 2048), F32)

    @pl.when(l == 31)
    def _():
        halo[1] = jnp.zeros((8, 2048), F32)

    arrived(halo.at[0], h_recv.at[0], h_send.at[0], at_lat(south_of), l > 0)
    arrived(halo.at[1], h_recv.at[1], h_send.at[1], at_lat(north_of), l < 31)
    low, high = halo[0], halo[1]
    beyond_low = jnp.where(l > 0, advanced(None, low, tile(xb, 0)), 0.0)
    edge = advanced(low, tile(xb, 0), tile(xb, 1))
    x1b[0:8, :] = edge
    finish_tile(0, advanced(beyond_low, edge, tile(x1b, 1)))
    beyond_high = jnp.where(l < 31, advanced(tile(xb, 3), high, None), 0.0)
    edge = advanced(tile(xb, 2), tile(xb, 3), high)
    x1b[24:32, :] = edge
    finish_tile(3, advanced(tile(x1b, 2), edge, beyond_high))
    send_a(1)
    for g in range(4):
        send(x2b.at[g], pb.at[g], e_send.at[g], e_recv.at[g], at_win(lax.rem(w + 1, 16)), w < 15)
    a_in[w] = a_out[w]

    loads[2].wait()
    loads[3].wait()
    for t in range(4):
        rows = slice(8 * t, 8 * t + 8)
        second = jnp.concatenate([x2b[g, rows, :] for g in range(4)], axis=1)
        lb[rows, :] = (
            kb[0, rows, :].astype(F32) * (ob[0, rows, :] - x1b[rows, :])
            + kb[1, rows, :].astype(F32) * (ob[1, rows, :] - second)
            + (mb[rows, :] + later * xb[rows, :])
        )

    for k in range(1, 16):
        v = lax.rem(w + k, 16)
        arrived(a_in.at[v], a_recv.at[v], a_send.at[v], at_win(v))
    total = jnp.zeros((8, 512), F32)
    for v in range(16):
        p_out[v] = total
        if v < 15:
            total = total + a_in[v]
    for off in AROUND:
        for far in (1, 0):
            if off or far:
                v = lax.rem(xh + far, 2) * 8 + lax.rem(y + off, 8)
                send(p_out.at[v], p_in.at[w], p_send.at[v], p_recv.at[w], at_win(v))
    p_in[w] = p_out[w]

    for load in loads[4:]:
        load.wait()
    for ref, out, n1, n2, scale in ((ls, lsf, 32, 32, 2.0**-22), (lo, lnf, 16, 128, 1.0)):
        spread = gathered(ref[...], n1, n2) * scale
        depth = 512 // n1
        for k in range(n1):
            out[depth * k : depth * (k + 1), :] = jnp.broadcast_to(spread[k : k + 1, :], (depth, 128))

    @pl.when(w == 0)
    def _():
        pb[...] = jnp.zeros((4, 32, 512), F32)

    for g in range(4):
        for t in range(4):
            owner = slot_of(t, g)
            arrived(p_in.at[owner], p_recv.at[owner], p_send.at[owner], at_win(owner * 1 + 0 * w), w != owner)
        arrived(pb.at[g], e_recv.at[g], e_send.at[g], at_win(lax.rem(w + 15, 16)), w > 0)
        columns = slice(512 * g, 512 * g + 512)
        for t in range(4):
            rows = slice(8 * t, 8 * t + 8)
            prior = 0.5 * pb[g, rows, :]
            lamb[rows, columns] = mb[rows, columns] + later * xb[rows, columns] - prior
            r = lb[rows, columns] - prior - (p_in[slot_of(t, g)] + prior) * inv
            for c in range(4):
                rb[32 * c + 8 * t : 32 * c + 8 * t + 8, :] = r[:, 128 * c : 128 * c + 128]
        tb[g] = rb[...].T
        for off in AROUND:
            to = lax.rem(z + off, 8)
            target = to * 4 + g
            when = None if off else (group != g)
            send(
                tb.at[g, pl.ds(pl.multiple_of(to * 16, 16), 16), :], zb.at[l],
                z_send.at[target], z_recv.at[l], at_lat(target), when,
            )
    zb[l] = tb[group, pl.ds(pl.multiple_of(z * 16, 16), 16), :]
    save = pltpu.make_async_copy(lamb, new_mult, out_sem.at[0])
    save.start()

    for k in range(1, 32):
        m = lax.rem(l + k, 32)
        arrived(zb.at[m], z_recv.at[m], z_send.at[m], at_lat(m))

    def operator(n1, depth, source, sink, cos_at, sin_at, table, scale):
        cos = [twb[cos_at + k : cos_at + k + 1, :] for k in range(n1)]
        sin = [twb[sin_at + k : sin_at + k + 1, :] for k in range(n1)]
        for h in range(depth // 8):
            u, v = analyse([source(j, h) for j in range(n1)], cos, sin)
            for k in range(n1):
                at = depth * k + 8 * h
                uv[at : at + 8, 0:128] = u[k]
                uv[at : at + 8, 128:256] = v[k]
        for q in range(4):
            rows = slice(128 * q, 128 * q + 128)
            spectral = dot3(uv[rows, :], wfb[table, 0], wfb[table, 1]) * scale[rows, :]
            uv[rows, :] = dot3(spectral, wbb[table, 0], wbb[table, 1])
        for h in range(depth // 8):
            at = [depth * k + 8 * h for k in range(n1)]
            out = synthesise([uv[a : a + 8, 0:128] for a in at], [uv[a : a + 8, 128:256] for a in at], cos, sin)
            for j in range(n1):
                sink(j, h, out[j])

    def lat_sink(j, h, value):
        ob2[j, 8 * h : 8 * h + 8, :] = value

    operator(32, 16, lambda j, h: zb[j, 8 * h : 8 * h + 8, :], lat_sink, 0, 32, 0, lsf)
    here = pl.ds(pl.multiple_of(z * 16, 16), 16)
    for off in AROUND:
        for near in (2, 3, 1, 0):
            if off or near:
                m = lax.rem(z + off, 8) * 4 + lax.rem(group + near, 4)
                send(ob2.at[m], yb.at[group, here, :], y_send.at[m], y_recv.at[l], at_lat(m))
    yb[group, here, :] = ob2[l]

    for k in range(1, 32):
        m = lax.rem(l + k, 32)
        there = pl.ds(pl.multiple_of(lax.div(m, 4) * 16, 16), 16)
        arrived(yb.at[lax.rem(m, 4), there, :], y_recv.at[m], y_send.at[m], at_lat(m))
    for g in range(4):
        turned = yb[g].T
        for c in range(4):
            vb[4 * g + c] = turned[32 * c : 32 * c + 32, :]

    def lon_sink(j, h, value):
        rows, columns = slice(8 * h, 8 * h + 8), slice(128 * j, 128 * j + 128)
        outb[rows, columns] = xb[rows, columns] + value

    operator(16, 32, lambda j, h: vb[j, 8 * h : 8 * h + 8, :], lon_sink, 64, 80, 1, lnf)
    result = pltpu.make_async_copy(outb, new_state, out_sem.at[1])
    result.start()
    for when, copy in sends:
        guarded(when, copy.wait_send)
    save.wait()
    result.wait()


def per_device(state, multipliers, observations, obs_mask, speed, drift, kappa, lat_spectrum, lon_spectrum):
    band, nlon = state.shape[2:]
    tw_lat, w_lat = tables(32, 32)
    tw_lon, w_lon = tables(16, 128)
    tw = jnp.asarray(np.concatenate([tw_lat, tw_lon], 0))
    wf = jnp.asarray(np.stack([halves(w_lat), halves(w_lon)]))
    wb = jnp.asarray(np.stack([halves(np.ascontiguousarray(w_lat.T)), halves(np.ascontiguousarray(w_lon.T))]))
    hbm = pl.BlockSpec(memory_space=pltpu.HBM)
    smem = pl.BlockSpec(memory_space=pltpu.SMEM)
    vmem = pltpu.VMEM
    dma = pltpu.SemaphoreType.DMA
    new_state, new_mult = pl.pallas_call(
        kernel,
        out_shape=[jax.ShapeDtypeStruct((band, nlon), F32)] * 2,
        in_specs=[hbm] * 4 + [smem] * 3 + [hbm] * 5,
        out_specs=[hbm] * 2,
        scratch_shapes=[
            vmem((32, 2048), F32), vmem((32, 2048), F32), vmem((2, 32, 2048), F32), vmem((2, 32, 2048), jnp.int32),
            vmem((1, 1024), F32), vmem((1, 2048), F32), vmem((96, 128), F32),
            vmem((2, 2, 256, 128), BF16), vmem((2, 2, 128, 256), BF16),
            vmem((2, 8, 2048), F32), vmem((32, 2048), F32), vmem((4, 32, 512), F32), vmem((4, 32, 512), F32),
            vmem((32, 2048), F32), vmem((32, 2048), F32),
            vmem((16, 8, 512), F32), vmem((16, 8, 512), F32), vmem((16, 8, 512), F32), vmem((16, 8, 512), F32),
            vmem((128, 128), F32), vmem((4, 128, 128), F32), vmem((32, 16, 128), F32),
            vmem((4, 128, 128), F32), vmem((32, 16, 128), F32), vmem((16, 32, 128), F32), vmem((512, 256), F32),
            vmem((512, 128), F32), vmem((512, 128), F32), vmem((32, 2048), F32),
            dma((9,)), dma((2,)), dma((2,)), dma((2,)), dma((16,)), dma((16,)), dma((16,)), dma((16,)),
            dma((4,)), dma((4,)), dma((32,)), dma((32,)), dma((32,)), dma((32,)),
        ],
        compiler_params=pltpu.CompilerParams(
            collective_id=0, has_side_effects=True, vmem_limit_bytes=40 * 1024 * 1024
        ),
        name="saddle_step",
    )(
        state[0, 0], multipliers[0, 0], observations[0, :, 0], obs_mask[0], speed, drift, kappa,
        lat_spectrum, lon_spectrum, tw, wf, wb,
    )
    return new_state[None, None], new_mult[None, None]


def solution(mesh):
    finer = Mesh(mesh.devices.reshape(2, 8, 8, 2, 2), AXES)
    placed = (
        P(WIN, None, LAT, None),
        P(WIN, None, LAT, None),
        P(WIN, None, None, LAT, None),
        P(WIN, None, LAT, None),
        P(),
        P(),
        P(),
        P(),
        P(),
    )
    return jax.shard_map(
        per_device,
        mesh=finer,
        in_specs=placed,
        out_specs=(P(WIN, None, LAT, None), P(WIN, None, LAT, None)),
        check_vma=False,
    )
```

```python
import functools
import math

import jax
import jax.numpy as jnp
import numpy as np
from jax import lax
from jax.experimental import pallas as pl
from jax.experimental.pallas import tpu as pltpu
from jax.sharding import Mesh
from jax.sharding import PartitionSpec as P

AXES = ("win_0", "win_1", "lat_0", "lat_1", "lat_2")
WIN = AXES[:2]
LAT = AXES[2:]
F32 = jnp.float32
BF16 = jnp.bfloat16
AROUND = (4, 5, 3, 6, 2, 7, 1, 0)
TILE_OF = (1, 0, 2, 3)


def rotated(c, s, angle):
    if s is None:
        return c * math.cos(angle), c * math.sin(angle)
    cos, sin = math.cos(angle), math.sin(angle)
    return c * cos - s * sin, c * sin + s * cos


def rfft(xs):
    n = len(xs)
    if n == 2:
        return [(xs[0] + xs[1], None), (xs[0] - xs[1], None)]
    even, odd = rfft(xs[0::2]), rfft(xs[1::2])
    out = [None] * (n // 2 + 1)
    for k in range(n // 4 + 1):
        (ec, es), (oc, os) = even[k], odd[k]
        if k == 0:
            out[0] = (ec + oc, None)
            out[n // 2] = (ec - oc, None)
        elif k == n // 4:
            out[k] = (ec, oc)
        else:
            tc, ts = rotated(oc, os, 2 * math.pi * k / n)
            if es is None:
                out[k] = (ec + tc, ts)
                out[n // 2 - k] = (ec - tc, ts)
            else:
                out[k] = (ec + tc, es + ts)
                out[n // 2 - k] = (ec - tc, ts - es)
    return out


def synth(n, c, s):
    if n == 2:
        return [c[0] + c[1], c[0] - c[1]]
    half, quarter = n // 2, n // 4
    ec, es, oc, os = [], [], [], []
    for k in range(quarter + 1):
        if k == quarter:
            ec.append(c[k])
            es.append(None)
            oc.append(s[k])
            os.append(None)
        elif k == 0:
            ec.append(c[0] + c[half])
            es.append(None)
            oc.append(c[0] - c[half])
            os.append(None)
        else:
            cos, sin = math.cos(2 * math.pi * k / n), math.sin(2 * math.pi * k / n)
            ec.append(c[k] + c[half - k])
            es.append(s[k] - s[half - k])
            dc, ds = c[k] - c[half - k], s[k] + s[half - k]
            oc.append(dc * cos + ds * sin)
            os.append(ds * cos - dc * sin)
    out = [None] * n
    out[0::2] = synth(half, ec, es)
    out[1::2] = synth(half, oc, os)
    return out


def analyse(xs, cos, sin):
    n = len(xs)
    bins = rfft(xs)
    u, v = [], []
    for k in range(n):
        c, s = bins[k] if k <= n // 2 else bins[n - k]
        if k == 0:
            u.append(c)
            v.append(c * 0.0)
        elif s is None:
            u.append(c * cos[k])
            v.append(c * sin[k])
        elif k <= n // 2:
            u.append(c * cos[k] - s * sin[k])
            v.append(c * sin[k] + s * cos[k])
        else:
            u.append(c * cos[k] + s * sin[k])
            v.append(c * sin[k] - s * cos[k])
    return u, v


def synthesise(u, v, cos, sin):
    n = len(u)
    c, s = [u[0]], [None]
    for k in range(1, n):
        c.append(u[k] * cos[k] + v[k] * sin[k])
        s.append(None if k == n // 2 else v[k] * cos[k] - u[k] * sin[k])
    half = n // 2
    fc = [c[0]] + [c[k] + c[n - k] for k in range(1, half)] + [c[half]]
    fs = [None] + [s[k] - s[n - k] for k in range(1, half)] + [None]
    return synth(n, fc, fs)


def twiddle(n1, n2):
    angle = 2 * np.pi * np.arange(n1)[:, None] * np.arange(n2)[None] / (n1 * n2)
    return np.cos(angle), np.sin(angle)


def casmat(n2):
    angle = 2 * np.pi * (np.arange(n2)[:, None] * np.arange(n2)[None] % n2) / n2
    cos, sin = np.cos(angle), np.sin(angle)
    return np.concatenate([cos + sin, cos - sin], 0)


def tables(n1, n2):
    copies = 128 // n2
    cos, sin = (np.tile(t, (1, copies)) for t in twiddle(n1, n2))
    one = casmat(n2)
    eye = np.eye(copies)
    full = np.concatenate([np.kron(eye, one[:n2]), np.kron(eye, one[n2:])], 0)
    return np.concatenate([cos, sin], 0).astype(np.float32), full.astype(np.float32)


def halves(full):
    import ml_dtypes

    hi = full.astype(ml_dtypes.bfloat16)
    lo = (full - hi.astype(np.float32)).astype(ml_dtypes.bfloat16)
    return np.stack([hi, lo])


def dot3(a, hi, lo):
    a_hi = a.astype(BF16)
    a_lo = (a - a_hi.astype(F32)).astype(BF16)
    dot = functools.partial(jnp.dot, preferred_element_type=F32)
    return dot(a_hi, hi) + (dot(a_lo, hi) + dot(a_hi, lo))


def gathered(spec, n1, n2):
    n = n1 * n2
    rows = lax.broadcasted_iota(jnp.int32, (n1, n), 0)
    lanes = lax.broadcasted_iota(jnp.int32, (n1, n), 1)
    own = jnp.where((lanes & (n1 - 1)) == rows, jnp.broadcast_to(spec, (n1, n)), 0.0)
    first = own.astype(BF16)
    rest = own - first.astype(F32)
    second = rest.astype(BF16)
    third = (rest - second.astype(F32)).astype(BF16)
    place = lax.broadcasted_iota(jnp.int32, (n, 128), 0) >> (n1.bit_length() - 1)
    lane = lax.broadcasted_iota(jnp.int32, (n, 128), 1) & (n2 - 1)
    pick = jnp.where(place == lane, 1.0, 0.0).astype(BF16)
    dot = functools.partial(jnp.dot, preferred_element_type=F32)
    return dot(first, pick) + dot(second, pick) + dot(third, pick)


def slot_of(tile, group):
    return (group // 2) * 8 + (group % 2) * 4 + TILE_OF.index(tile)


def operator(source, sink, n1, depth, cos, sin, scale, uv, wf, wb):
    for h in range(depth // 8):
        u, v = analyse([source(j, h) for j in range(n1)], cos, sin)
        for k in range(n1):
            at = depth * k + 8 * h
            uv[at : at + 8, 0:128] = u[k]
            uv[at : at + 8, 128:256] = v[k]
    for q in range(4):
        rows = slice(128 * q, 128 * q + 128)
        factor = jnp.concatenate(
            [jnp.broadcast_to(scale[k : k + 1, :], (depth, 128)) for k in range(128 * q // depth, 128 * (q + 1) // depth)], axis=0
        )
        spectral = dot3(uv[rows, :], wf[0], wf[1]) * factor
        uv[rows, :] = dot3(spectral, wb[0], wb[1])
    for h in range(depth // 8):
        at = [depth * k + 8 * h for k in range(n1)]
        out = synthesise([uv[a : a + 8, 0:128] for a in at], [uv[a : a + 8, 128:256] for a in at], cos, sin)
        for j in range(n1):
            sink(j, h, out[j])


def rows_of(ref, first, count):
    return [ref[first + k : first + k + 1, :] for k in range(count)]


def exchange_kernel(
    state, mult, obs, mask, speed, drift, kappa, lat_spec, lon_spec, tw, wf, wb,
    turned, new_mult, lon_scale,
    xb, mb, ob, kb, ls, lo, twb, wfb, wbb,
    halo, x1b, x2b, pb, lb, lamb, a_out, a_in, p_out, p_in, ea_out, ea_in, ep_out, ep_in, rel,
    rb, tb, zb, ob2, uv, lsf, lnf,
    in_sem, out_sem, h_send, h_recv, a_send, a_recv, p_send, p_recv, ea_send, ea_recv, ep_send, ep_recv,
    e_send, e_recv, rel_send, rel_recv, z_send, z_recv, y_send, y_recv,
):
    xh, y, z, xl, core = (lax.axis_index(a) for a in AXES)
    w = xh * 8 + y
    l = z * 4 + xl * 2 + core
    group = xl * 2 + core

    def at_win(v):
        return (lax.div(v, 8), lax.rem(v, 8), z, xl, core)

    def at_lat(m):
        return (xh, y, lax.div(m, 4), lax.rem(lax.div(m, 2), 2), lax.rem(m, 2))

    loads = [
        pltpu.make_async_copy(src, dst, in_sem.at[i])
        for i, (src, dst) in enumerate(
            [(state, xb), (mult, mb), (obs, ob), (mask, kb), (lat_spec, ls), (lon_spec, lo), (tw, twb), (wf, wfb), (wb, wbb)]
        )
    ]
    for load in loads:
        load.start()

    windows = [lax.rem(xh + far, 2) * 8 + lax.rem(y + off, 8) for off in AROUND for far in (1, 0) if off or far]
    bands = [lax.rem(z + off, 8) * 4 + lax.rem(group + near, 4) for off in AROUND for near in (2, 3, 1, 0) if off or near]
    barrier = pltpu.get_barrier_semaphore()
    for v in windows:
        pl.semaphore_signal(barrier, inc=1, device_id=at_win(v), device_id_type=pl.DeviceIdType.MESH)
    for m in bands:
        pl.semaphore_signal(barrier, inc=1, device_id=at_lat(m), device_id_type=pl.DeviceIdType.MESH)

    def guarded(when, act):
        if when is None:
            act()
        else:
            pl.when(when)(act)

    def send(src, dst, send_sem, recv_sem, device, when=None):
        copy = pltpu.make_async_remote_copy(
            src_ref=src, dst_ref=dst, send_sem=send_sem, recv_sem=recv_sem,
            device_id=device, device_id_type=pl.DeviceIdType.MESH,
        )
        guarded(when, copy.start)

    def wait(like, sem, when=None):
        guarded(when, pltpu.make_async_copy(like, like, sem).wait)

    def wait_either(when, first, second, sem):
        wait(first, sem, when)
        wait(second, sem, jnp.logical_not(when))

    row = lax.broadcasted_iota(jnp.int32, (8, 2048), 0)
    row8 = lax.broadcasted_iota(jnp.int32, (8, 1024), 0)
    row1 = lax.broadcasted_iota(jnp.int32, (8, 128), 0)
    later = jnp.where(w > 0, F32(0.5), F32(0.0))
    inv = F32(1.0)
    for k in range(2, 16):
        inv = jnp.where(w == k, F32(1.0 / k), inv)
    sp, dr, ka = speed[0], drift[0], kappa[0]

    def step(mid, north, south):
        east = pltpu.roll(mid, 2047, 1)
        west = pltpu.roll(mid, 1, 1)
        return (
            mid
            - (sp * mid * (east - west)) * 0.5
            - (dr * (north - south)) * 0.5
            + ka * (east + west + north + south - 4.0 * mid)
        )

    def advanced(before, mid, after):
        north, south = pltpu.roll(mid, 7, 0), pltpu.roll(mid, 1, 0)
        if after is not None:
            north = jnp.where(row == 7, pltpu.roll(after, 7, 0), north)
        if before is not None:
            south = jnp.where(row == 0, pltpu.roll(before, 1, 0), south)
        return step(mid, north, south)

    def tile(ref, t):
        return ref[8 * t : 8 * t + 8, :]

    def keep(t, second):
        for g in range(4):
            for q in range(4):
                at = 512 * g + 128 * q
                x2b[q, 8 * t : 8 * t + 8, 128 * g : 128 * g + 128] = second[:, at : at + 128]

    def term(t, second):
        return tile(mb, t) + later * tile(xb, t) - 0.5 * second

    def send_prior(q, when):
        send(x2b.at[q], pb.at[q], e_send, e_recv.at[q], at_win(lax.rem(w + 1, 16)), when)

    def relay_prior():
        wait(rel, rel_recv)
        for q in (2, 3):
            send(rel.at[q - 2], pb.at[q], rel_send, e_recv.at[q], at_win(jnp.int32(8)))

    loads[0].wait()
    first = [tile(xb, t) for t in range(4)]
    for t in range(4):
        x1b[8 * t : 8 * t + 8, :] = advanced(
            first[t - 1] if t > 0 else None, first[t], first[t + 1] if t < 3 else None
        )
    loads[1].wait()
    for t in range(4):
        second = advanced(
            tile(x1b, t - 1) if t > 0 else None, tile(x1b, t), tile(x1b, t + 1) if t < 3 else None
        )
        if t in (1, 2):
            keep(t, second)
        a = term(t, second)
        for g in range(4):
            for s in range(2):
                a_out[16 * s + slot_of(t, g)] = a[:, 512 * g + 256 * s : 512 * g + 256 * s + 256]
    pl.semaphore_wait(barrier, 46)
    north_of, south_of = lax.rem(l + 1, 32), lax.rem(l + 31, 32)
    send(xb.at[24:32, :], halo.at[0], h_send.at[0], h_recv.at[0], at_lat(north_of), l < 31)
    send(xb.at[0:8, :], halo.at[1], h_send.at[1], h_recv.at[1], at_lat(south_of), l > 0)

    def send_a(s, some):
        for v in some:
            send(a_out.at[16 * s + v], a_in.at[s, w], a_send, a_recv.at[s], at_win(v), w < 15)

    send_a(0, windows)
    send_a(1, windows[:7])
    for s in range(2):
        a_in[s, w] = a_out[16 * s + w]

    @pl.when(l == 0)
    def _():
        halo[0] = jnp.zeros((8, 2048), F32)

    @pl.when(l == 31)
    def _():
        halo[1] = jnp.zeros((8, 2048), F32)

    @pl.when(w == 0)
    def _():
        pb[...] = jnp.zeros(pb.shape, F32)
        p_in[...] = jnp.zeros(p_in.shape, F32)
        ep_in[...] = jnp.zeros(ep_in.shape, F32)

    wait(halo.at[0], h_recv.at[0], l > 0)
    wait(halo.at[1], h_recv.at[1], l < 31)
    low, high = halo[0], halo[1]
    beyond_low = jnp.where(l > 0, advanced(None, low, tile(xb, 0)), 0.0)
    edge = advanced(low, tile(xb, 0), tile(xb, 1))
    x1b[0:8, :] = edge
    bottom = advanced(beyond_low, edge, tile(x1b, 1))
    beyond_high = jnp.where(l < 31, advanced(tile(xb, 3), high, None), 0.0)
    edge = advanced(tile(xb, 2), tile(xb, 3), high)
    x1b[24:32, :] = edge
    top = advanced(tile(x1b, 2), edge, beyond_high)
    keep(0, bottom)
    keep(3, top)
    outer = jnp.where(row < 4, term(0, bottom), term(3, top))
    packed = jnp.where((row8 < 2) | (row8 >= 6), outer[:, :1024], pltpu.roll(outer[:, 1024:], 4, 0))
    holder = lax.rem(y, 2) == xh
    for k in range(8):
        ea_out[k] = packed[:, 128 * k : 128 * k + 128]
    for off in AROUND:
        k = lax.rem(y + off, 8)
        v = lax.rem(k, 2) * 8 + k
        send(ea_out.at[k], ea_in.at[w], ea_send, ea_recv, at_win(v), jnp.logical_and(w < 15, w != v))
    send_a(1, windows[7:])
    ea_in[w] = ea_out[y]
    send_prior(0, w < 15)
    for q in (2, 3):
        send(x2b.at[q], rel.at[q - 2], e_send, rel_recv, at_win(jnp.int32(15)), w == 7)
    send_prior(1, w == 7)

    loads[2].wait()
    loads[3].wait()
    for t in range(4):
        rows = slice(8 * t, 8 * t + 8)
        for g in range(4):
            for q in range(4):
                at = slice(512 * g + 128 * q, 512 * g + 128 * q + 128)
                u = mb[rows, at] + later * xb[rows, at]
                lamb[rows, at] = u
                lb[rows, at] = (
                    kb[0, rows, at].astype(F32) * (ob[0, rows, at] - x1b[rows, at])
                    + kb[1, rows, at].astype(F32) * (ob[1, rows, at] - x2b[q, rows, 128 * g : 128 * g + 128])
                    + u
                )

    def piece(s):
        wait_either(w == 15, a_in.at[s, 0:15], a_in.at[s, 0:14], a_recv.at[s])
        total = jnp.zeros((8, 256), F32)
        for v in range(16):
            p_out[32 * s + v] = total[:, :128]
            p_out[32 * s + 16 + v] = total[:, 128:]
            if v < 15:
                total = total + a_in[s, v]
        for q in (2 * s, 2 * s + 1):
            for v in windows:
                send(p_out.at[16 * q + v], p_in.at[q, w], p_send, p_recv.at[q], at_win(v), v > 0)
            if q > 0:
                send_prior(q, jnp.logical_and(w < 15, w != 7))
        for q in (2 * s, 2 * s + 1):
            p_in[q, w] = p_out[16 * q + w]

    piece(0)

    @pl.when(holder)
    def _():
        wait_either(w == 15, ea_in.at[0:15], ea_in.at[0:14], ea_recv)
        total = jnp.zeros((8, 128), F32)
        for v in range(16):
            ep_out[v] = total
            if v < 15:
                total = total + ea_in[v]
        for v in windows:
            send(ep_out.at[v], ep_in.at[y], ep_send, ep_recv, at_win(v), v > 0)
        ep_in[y] = ep_out[w]

    piece(1)
    pl.when(w == 15)(relay_prior)

    for load in loads[4:]:
        load.wait()
    lsf[...] = gathered(ls[...], 32, 32) * 2.0**-22
    lnf[...] = gathered(lo[...], 16, 128)
    save_scale = pltpu.make_async_copy(lnf, lon_scale, out_sem.at[0])
    save_scale.start()

    @pl.when(w > 0)
    def _():
        wait_either(holder, ep_in.at[0:7], ep_in.at[0:8], ep_recv)

    for q in range(4):
        wait(p_in.at[q, 0:15], p_recv.at[q], w > 0)
        wait(pb.at[q], e_recv.at[q], w > 0)
        for g in range(4):
            at = slice(512 * g + 128 * q, 512 * g + 128 * q + 128)
            outer = ep_in[4 * (g % 2) + q]
            if g >= 2:
                outer = pltpu.roll(outer, 4, 0)
            for t in range(4):
                rows = slice(8 * t, 8 * t + 8)
                prior = 0.5 * pb[q, rows, 128 * g : 128 * g + 128]
                lamb[rows, at] = lamb[rows, at] - prior
                earlier = p_in[q, slot_of(t, g)]
                if t == 0:
                    earlier = jnp.where(row1 < 2, outer, earlier)
                if t == 3:
                    earlier = jnp.where(row1 >= 6, outer, earlier)
                rb[32 * g + 8 * t : 32 * g + 8 * t + 8, :] = lb[rows, at] - prior - (earlier + prior) * inv
        tb[q] = rb[...].T
        for off in AROUND:
            to = lax.rem(z + off, 8)
            target = to * 4 + q
            when = None if off else (group != q)
            send(tb.at[q, pl.ds(pl.multiple_of(to * 16, 16), 16), :], zb.at[l], z_send, z_recv, at_lat(target), when)
    here = pl.ds(pl.multiple_of(z * 16, 16), 16)
    zb[l] = tb[group, here, :]
    save = pltpu.make_async_copy(lamb, new_mult, out_sem.at[1])
    save.start()

    wait(zb.at[0:31], z_recv)

    def sink(j, h, value):
        ob2[j, 8 * h : 8 * h + 8, :] = value

    operator(
        lambda j, h: zb[j, 8 * h : 8 * h + 8, :], sink, 32, 16, rows_of(twb, 0, 32), rows_of(twb, 32, 32), lsf, uv, wfb, wbb
    )
    for m in bands:
        send(ob2.at[m], turned.at[group, here, :], y_send, y_recv, at_lat(m))
    own = pltpu.make_async_copy(ob2.at[l], turned.at[group, here, :], out_sem.at[2])
    own.start()

    wait(halo.at[0], h_send.at[0], l < 31)
    wait(halo.at[1], h_send.at[1], l > 0)

    @pl.when(w < 15)
    def _():
        wait(a_out.at[0:30], a_send)
        wait(x2b, e_send)
        wait_either(holder, ea_out.at[0:7], ea_out.at[0:8], ea_send)

    wait_either(w == 0, p_out.at[0:60], p_out.at[0:56], p_send)

    @pl.when(holder)
    def _():
        wait_either(w == 0, ep_out.at[0:15], ep_out.at[0:14], ep_send)

    wait(rel, rel_send, w == 15)
    wait(zb.at[0:31], z_send)
    save_scale.wait()
    save.wait()
    own.wait()
    wait(ob2.at[0:31], y_send)
    wait(ob2.at[0:31], y_recv)


def longitude_kernel(
    state, lam, turned, lon_scale, tw, wf, wb,
    new_state, new_mult,
    xb, lamb, yb, lnf, twb, wfb, wbb, vb, uv, outb, in_sem, out_sem,
):
    loads = [
        pltpu.make_async_copy(src, dst, in_sem.at[i])
        for i, (src, dst) in enumerate(
            [(turned, yb), (tw, twb), (wf, wfb), (lon_scale, lnf), (wb, wbb), (state, xb), (lam, lamb)]
        )
    ]
    for load in loads:
        load.start()
    loads[0].wait()
    loads[1].wait()
    for q in range(4):
        flat = yb[q].T
        for g in range(4):
            vb[4 * g + q] = flat[32 * g : 32 * g + 32, :]
    for load in loads[2:]:
        load.wait()
    save = pltpu.make_async_copy(lamb, new_mult, out_sem.at[0])
    save.start()

    def sink(j, h, value):
        rows, columns = slice(8 * h, 8 * h + 8), slice(128 * j, 128 * j + 128)
        outb[rows, columns] = xb[rows, columns] + value

    operator(lambda j, h: vb[j, 8 * h : 8 * h + 8, :], sink, 16, 32, rows_of(twb, 0, 16), rows_of(twb, 16, 16), lnf, uv, wfb, wbb)
    result = pltpu.make_async_copy(outb, new_state, out_sem.at[1])
    result.start()
    save.wait()
    result.wait()


def per_device(state, multipliers, observations, obs_mask, speed, drift, kappa, lat_spectrum, lon_spectrum):
    band, nlon = state.shape[2:]
    (tw_lat, w_lat), (tw_lon, w_lon) = tables(32, 32), tables(16, 128)
    hbm = pl.BlockSpec(memory_space=pltpu.HBM)
    vmem = pltpu.VMEM
    dma = pltpu.SemaphoreType.DMA
    grid = jax.ShapeDtypeStruct((band, nlon), F32)
    field = vmem((32, 2048), F32)
    turned, lam, lon_scale = pl.pallas_call(
        exchange_kernel,
        out_shape=[jax.ShapeDtypeStruct((4, 128, 128), F32), grid, jax.ShapeDtypeStruct((16, 128), F32)],
        in_specs=[hbm] * 4 + [pl.BlockSpec(memory_space=pltpu.SMEM)] * 3 + [hbm] * 5,
        out_specs=[hbm] * 3,
        scratch_shapes=[
            field, field, vmem((2, 32, 2048), F32), vmem((2, 32, 2048), jnp.int32),
            vmem((1, 1024), F32), vmem((1, 2048), F32), vmem((64, 128), F32), vmem((2, 256, 128), BF16), vmem((2, 128, 256), BF16),
            vmem((2, 8, 2048), F32), field, vmem((4, 32, 512), F32), vmem((4, 32, 512), F32), field, field,
            vmem((32, 8, 256), F32), vmem((2, 16, 8, 256), F32), vmem((64, 8, 128), F32), vmem((4, 16, 8, 128), F32),
            vmem((8, 8, 128), F32), vmem((16, 8, 128), F32), vmem((16, 8, 128), F32), vmem((8, 8, 128), F32), vmem((2, 32, 512), F32),
            vmem((128, 128), F32), vmem((4, 128, 128), F32), vmem((32, 16, 128), F32), vmem((32, 16, 128), F32),
            vmem((512, 256), F32), vmem((32, 128), F32), vmem((16, 128), F32),
            dma((9,)), dma((3,)), dma((2,)), dma((2,)), dma, dma((2,)), dma, dma((4,)),
            dma, dma, dma, dma, dma, dma((4,)), dma, dma, dma, dma, dma, dma,
        ],
        compiler_params=pltpu.CompilerParams(collective_id=0, has_side_effects=True, vmem_limit_bytes=67043328),
        name="exchange",
    )(
        state[0, 0], multipliers[0, 0], observations[0, :, 0], obs_mask[0], speed, drift, kappa, lat_spectrum, lon_spectrum,
        jnp.asarray(tw_lat), jnp.asarray(halves(w_lat)), jnp.asarray(halves(np.ascontiguousarray(w_lat.T))),
    )
    new_state, new_mult = pl.pallas_call(
        longitude_kernel,
        out_shape=[grid] * 2,
        in_specs=[hbm] * 7,
        out_specs=[hbm] * 2,
        scratch_shapes=[
            field, field, vmem((4, 128, 128), F32), vmem((16, 128), F32), vmem((32, 128), F32),
            vmem((2, 256, 128), BF16), vmem((2, 128, 256), BF16), vmem((16, 32, 128), F32), vmem((512, 256), F32), field,
            dma((7,)), dma((2,)),
        ],
        compiler_params=pltpu.CompilerParams(vmem_limit_bytes=67043328),
        name="longitudes",
    )(
        state[0, 0], lam, turned, lon_scale,
        jnp.asarray(tw_lon), jnp.asarray(halves(w_lon)), jnp.asarray(halves(np.ascontiguousarray(w_lon.T))),
    )
    return new_state[None, None], new_mult[None, None]


def solution(mesh):
    finer = Mesh(mesh.devices.reshape(2, 8, 8, 2, 2), AXES)
    placed = (
        P(WIN, None, LAT, None),
        P(WIN, None, LAT, None),
        P(WIN, None, None, LAT, None),
        P(WIN, None, LAT, None),
        P(),
        P(),
        P(),
        P(),
        P(),
    )
    return jax.shard_map(
        per_device,
        mesh=finer,
        in_specs=placed,
        out_specs=(P(WIN, None, LAT, None), P(WIN, None, LAT, None)),
        check_vma=False,
    )
```

```python
import functools
import math

import jax
import jax.numpy as jnp
import numpy as np
from jax import lax
from jax.experimental import pallas as pl
from jax.experimental.pallas import tpu as pltpu
from jax.sharding import Mesh
from jax.sharding import PartitionSpec as P

AXES = ("win_0", "win_1", "lat_0", "lat_1", "lat_2")
WIN = AXES[:2]
LAT = AXES[2:]
F32 = jnp.float32
BF16 = jnp.bfloat16
AROUND = (4, 5, 3, 6, 2, 7, 1, 0)
TILE_OF = (1, 0, 2, 3)
PARTS = 4


def rotated(c, s, angle):
    if s is None:
        return c * math.cos(angle), c * math.sin(angle)
    cos, sin = math.cos(angle), math.sin(angle)
    return c * cos - s * sin, c * sin + s * cos


def rfft(xs):
    n = len(xs)
    if n == 2:
        return [(xs[0] + xs[1], None), (xs[0] - xs[1], None)]
    even, odd = rfft(xs[0::2]), rfft(xs[1::2])
    out = [None] * (n // 2 + 1)
    for k in range(n // 4 + 1):
        (ec, es), (oc, os) = even[k], odd[k]
        if k == 0:
            out[0] = (ec + oc, None)
            out[n // 2] = (ec - oc, None)
        elif k == n // 4:
            out[k] = (ec, oc)
        else:
            tc, ts = rotated(oc, os, 2 * math.pi * k / n)
            if es is None:
                out[k] = (ec + tc, ts)
                out[n // 2 - k] = (ec - tc, ts)
            else:
                out[k] = (ec + tc, es + ts)
                out[n // 2 - k] = (ec - tc, ts - es)
    return out


def synth(n, c, s):
    if n == 2:
        return [c[0] + c[1], c[0] - c[1]]
    half, quarter = n // 2, n // 4
    ec, es, oc, os = [], [], [], []
    for k in range(quarter + 1):
        if k == quarter:
            ec.append(c[k])
            es.append(None)
            oc.append(s[k])
            os.append(None)
        elif k == 0:
            ec.append(c[0] + c[half])
            es.append(None)
            oc.append(c[0] - c[half])
            os.append(None)
        else:
            cos, sin = math.cos(2 * math.pi * k / n), math.sin(2 * math.pi * k / n)
            ec.append(c[k] + c[half - k])
            es.append(s[k] - s[half - k])
            dc, ds = c[k] - c[half - k], s[k] + s[half - k]
            oc.append(dc * cos + ds * sin)
            os.append(ds * cos - dc * sin)
    out = [None] * n
    out[0::2] = synth(half, ec, es)
    out[1::2] = synth(half, oc, os)
    return out


def analyse(xs, cos, sin):
    n = len(xs)
    bins = rfft(xs)
    u, v = [], []
    for k in range(n):
        c, s = bins[k] if k <= n // 2 else bins[n - k]
        if k == 0:
            u.append(c)
            v.append(c * 0.0)
        elif s is None:
            u.append(c * cos[k])
            v.append(c * sin[k])
        elif k <= n // 2:
            u.append(c * cos[k] - s * sin[k])
            v.append(c * sin[k] + s * cos[k])
        else:
            u.append(c * cos[k] + s * sin[k])
            v.append(c * sin[k] - s * cos[k])
    return u, v


def synthesise(u, v, cos, sin):
    n = len(u)
    c, s = [u[0]], [None]
    for k in range(1, n):
        c.append(u[k] * cos[k] + v[k] * sin[k])
        s.append(None if k == n // 2 else v[k] * cos[k] - u[k] * sin[k])
    half = n // 2
    fc = [c[0]] + [c[k] + c[n - k] for k in range(1, half)] + [c[half]]
    fs = [None] + [s[k] - s[n - k] for k in range(1, half)] + [None]
    return synth(n, fc, fs)


def twiddle(n1, n2):
    angle = 2 * np.pi * np.arange(n1)[:, None] * np.arange(n2)[None] / (n1 * n2)
    return np.cos(angle), np.sin(angle)


def casmat(n2):
    angle = 2 * np.pi * (np.arange(n2)[:, None] * np.arange(n2)[None] % n2) / n2
    cos, sin = np.cos(angle), np.sin(angle)
    return np.concatenate([cos + sin, cos - sin], 0)


def tables(n1, n2):
    copies = 128 // n2
    cos, sin = (np.tile(t, (1, copies)) for t in twiddle(n1, n2))
    one = casmat(n2)
    eye = np.eye(copies)
    full = np.concatenate([np.kron(eye, one[:n2]), np.kron(eye, one[n2:])], 0)
    return np.concatenate([cos, sin], 0).astype(np.float32), full.astype(np.float32)


def weights(full):
    import ml_dtypes

    first = full.astype(ml_dtypes.bfloat16)
    rest = (full - first.astype(np.float32)).astype(ml_dtypes.bfloat16)
    return np.concatenate([first, rest], 1), np.ascontiguousarray(np.concatenate([first.T, first.T, rest.T], 0))


def parted(a):
    first = a.astype(BF16)
    return first, (a - first.astype(F32)).astype(BF16)


def dot(a, b):
    return jnp.dot(a, b, preferred_element_type=F32)


def gathered(spec, n1, n2):
    n = n1 * n2
    rows = lax.broadcasted_iota(jnp.int32, (n1, n), 0)
    lanes = lax.broadcasted_iota(jnp.int32, (n1, n), 1)
    own = jnp.where((lanes & (n1 - 1)) == rows, jnp.broadcast_to(spec, (n1, n)), 0.0)
    first = own.astype(BF16)
    rest = own - first.astype(F32)
    second = rest.astype(BF16)
    third = (rest - second.astype(F32)).astype(BF16)
    place = lax.broadcasted_iota(jnp.int32, (n, 128), 0) >> (n1.bit_length() - 1)
    lane = lax.broadcasted_iota(jnp.int32, (n, 128), 1) & (n2 - 1)
    pick = jnp.where(place == lane, 1.0, 0.0).astype(BF16)
    return dot(first, pick) + dot(second, pick) + dot(third, pick)


def slot_of(tile, group):
    return (group // 2) * 8 + (group % 2) * 4 + TILE_OF.index(tile)


def operator(source, sink, n1, depth, cos, sin, scale, uv, wf, wb):
    for h in range(depth // 8):
        u, v = analyse([source(j, h) for j in range(n1)], cos, sin)
        for k in range(n1):
            at = depth * k + 8 * h
            uv[at : at + 8, 0:128] = u[k]
            uv[at : at + 8, 128:256] = v[k]
    count = 512 // PARTS
    for q in range(PARTS):
        rows = slice(count * q, count * (q + 1))
        factor = jnp.concatenate(
            [jnp.broadcast_to(scale[k : k + 1, :], (depth, 128)) for k in range(count * q // depth, count * (q + 1) // depth)],
            axis=0,
        )
        first, rest = parted(uv[rows, :])
        both = dot(first, wf[...])
        spectral = (both[:, :128] + (both[:, 128:] + dot(rest, wf[:, 0:128]))) * factor
        first, rest = parted(spectral)
        uv[rows, :] = dot(jnp.concatenate([first, rest], axis=1), wb[0:256, :]) + dot(first, wb[256:384, :])
    for h in range(depth // 8):
        at = [depth * k + 8 * h for k in range(n1)]
        out = synthesise([uv[a : a + 8, 0:128] for a in at], [uv[a : a + 8, 128:256] for a in at], cos, sin)
        for j in range(n1):
            sink(j, h, out[j])


def rows_of(ref, first, count):
    return [ref[first + k : first + k + 1, :] for k in range(count)]


def exchange_kernel(
    state, mult, obs, mask, speed, drift, kappa, lat_spec, lon_spec, tw, wf, wb,
    turned, new_mult, lon_scale,
    xb, mb, ob, kb, ls, lo, twb, wfb, wbb,
    halo, x1b, x2b, pb, lb, lamb, a_out, a_in, p_out, p_in, ea_out, ea_in, ep_out, ep_in, rel,
    rb, tb, zb, ob2, uv, lsf, lnf,
    in_sem, out_sem, h_send, h_recv, a_send, a_recv, p_send, p_recv, ea_send, ea_recv, ep_send, ep_recv,
    e_send, e_recv, rel_send, rel_recv, z_send, z_recv, y_send, y_recv,
):
    xh, y, z, xl, core = (lax.axis_index(a) for a in AXES)
    w = xh * 8 + y
    l = z * 4 + xl * 2 + core
    group = xl * 2 + core

    def at_win(v):
        return (lax.div(v, 8), lax.rem(v, 8), z, xl, core)

    def at_lat(m):
        return (xh, y, lax.div(m, 4), lax.rem(lax.div(m, 2), 2), lax.rem(m, 2))

    loads = [
        pltpu.make_async_copy(src, dst, in_sem.at[i])
        for i, (src, dst) in enumerate(
            [(state, xb), (mult, mb), (obs, ob), (mask, kb), (lat_spec, ls), (lon_spec, lo), (tw, twb), (wf, wfb), (wb, wbb)]
        )
    ]
    for load in loads:
        load.start()

    def ahead(place, off):
        return jnp.where(place + off >= 8, place + off - 8, place + off) if off else place

    windows, bands = [], []
    for off in AROUND:
        yy, zz = ahead(y, off), ahead(z, off)
        for xx in (1 - xh, xh):
            if off or xx is not xh:
                windows.append((xx * 8 + yy, (xx, yy, z, xl, core)))
        for xx, cc in ((1 - xl, core), (1 - xl, 1 - core), (xl, 1 - core), (xl, core)):
            if off or xx is not xl or cc is not core:
                bands.append((zz * 4 + xx * 2 + cc, (xh, y, zz, xx, cc)))
    barrier = pltpu.get_barrier_semaphore()
    for _, device in windows + bands:
        pl.semaphore_signal(barrier, inc=1, device_id=device, device_id_type=pl.DeviceIdType.MESH)

    def guarded(when, act):
        if when is None:
            act()
        else:
            pl.when(when)(act)

    def send(src, dst, send_sem, recv_sem, device, when=None):
        copy = pltpu.make_async_remote_copy(
            src_ref=src, dst_ref=dst, send_sem=send_sem, recv_sem=recv_sem,
            device_id=device, device_id_type=pl.DeviceIdType.MESH,
        )
        guarded(when, copy.start)

    def wait(like, sem, when=None):
        guarded(when, pltpu.make_async_copy(like, like, sem).wait)

    def wait_either(when, first, second, sem):
        wait(first, sem, when)
        wait(second, sem, jnp.logical_not(when))

    row = lax.broadcasted_iota(jnp.int32, (8, 2048), 0)
    row8 = lax.broadcasted_iota(jnp.int32, (8, 1024), 0)
    row1 = lax.broadcasted_iota(jnp.int32, (8, 128), 0)
    later = jnp.where(w > 0, F32(0.5), F32(0.0))
    inv = F32(1.0)
    for k in range(2, 16):
        inv = jnp.where(w == k, F32(1.0 / k), inv)
    sp, dr, ka = speed[0], drift[0], kappa[0]

    def step(mid, north, south):
        east = pltpu.roll(mid, 2047, 1)
        west = pltpu.roll(mid, 1, 1)
        return (
            mid
            - (sp * mid * (east - west)) * 0.5
            - (dr * (north - south)) * 0.5
            + ka * (east + west + north + south - 4.0 * mid)
        )

    def advanced(before, mid, after):
        north, south = pltpu.roll(mid, 7, 0), pltpu.roll(mid, 1, 0)
        if after is not None:
            north = jnp.where(row == 7, pltpu.roll(after, 7, 0), north)
        if before is not None:
            south = jnp.where(row == 0, pltpu.roll(before, 1, 0), south)
        return step(mid, north, south)

    def tile(ref, t):
        return ref[8 * t : 8 * t + 8, :]

    def keep(t, second):
        for g in range(4):
            for q in range(4):
                at = 512 * g + 128 * q
                x2b[q, 8 * t : 8 * t + 8, 128 * g : 128 * g + 128] = second[:, at : at + 128]

    def term(t, second):
        return tile(mb, t) + later * tile(xb, t) - 0.5 * second

    def send_prior(q, when):
        send(x2b.at[q], pb.at[q], e_send, e_recv.at[q], at_win(lax.rem(w + 1, 16)), when)

    def relay_prior():
        wait(rel, rel_recv)
        for q in (2, 3):
            send(rel.at[q - 2], pb.at[q], rel_send, e_recv.at[q], at_win(jnp.int32(8)))

    loads[0].wait()
    first = [tile(xb, t) for t in range(4)]
    for t in range(4):
        x1b[8 * t : 8 * t + 8, :] = advanced(
            first[t - 1] if t > 0 else None, first[t], first[t + 1] if t < 3 else None
        )
    loads[1].wait()
    for t in range(4):
        second = advanced(
            tile(x1b, t - 1) if t > 0 else None, tile(x1b, t), tile(x1b, t + 1) if t < 3 else None
        )
        if t in (1, 2):
            keep(t, second)
        a = term(t, second)
        for g in range(4):
            for s in range(2):
                a_out[16 * s + slot_of(t, g)] = a[:, 512 * g + 256 * s : 512 * g + 256 * s + 256]
    pl.semaphore_wait(barrier, 46)
    north_of, south_of = lax.rem(l + 1, 32), lax.rem(l + 31, 32)
    send(xb.at[24:32, :], halo.at[0], h_send.at[0], h_recv.at[0], at_lat(north_of), l < 31)
    send(xb.at[0:8, :], halo.at[1], h_send.at[1], h_recv.at[1], at_lat(south_of), l > 0)

    def send_a(s, some):
        for v, device in some:
            send(a_out.at[16 * s + v], a_in.at[s, w], a_send, a_recv.at[s], device, w < 15)

    send_a(0, windows)
    send_a(1, windows[:7])
    for s in range(2):
        a_in[s, w] = a_out[16 * s + w]

    @pl.when(l == 0)
    def _():
        halo[0] = jnp.zeros((8, 2048), F32)

    @pl.when(l == 31)
    def _():
        halo[1] = jnp.zeros((8, 2048), F32)

    @pl.when(w == 0)
    def _():
        pb[...] = jnp.zeros(pb.shape, F32)
        p_in[...] = jnp.zeros(p_in.shape, F32)
        ep_in[...] = jnp.zeros(ep_in.shape, F32)

    wait(halo.at[0], h_recv.at[0], l > 0)
    wait(halo.at[1], h_recv.at[1], l < 31)
    low, high = halo[0], halo[1]
    beyond_low = jnp.where(l > 0, advanced(None, low, tile(xb, 0)), 0.0)
    edge = advanced(low, tile(xb, 0), tile(xb, 1))
    x1b[0:8, :] = edge
    bottom = advanced(beyond_low, edge, tile(x1b, 1))
    beyond_high = jnp.where(l < 31, advanced(tile(xb, 3), high, None), 0.0)
    edge = advanced(tile(xb, 2), tile(xb, 3), high)
    x1b[24:32, :] = edge
    top = advanced(tile(x1b, 2), edge, beyond_high)
    keep(0, bottom)
    keep(3, top)
    outer = jnp.where(row < 4, term(0, bottom), term(3, top))
    packed = jnp.where((row8 < 2) | (row8 >= 6), outer[:, :1024], pltpu.roll(outer[:, 1024:], 4, 0))
    holder = lax.rem(y, 2) == xh
    for k in range(8):
        ea_out[k] = packed[:, 128 * k : 128 * k + 128]
    for off in AROUND:
        k = ahead(y, off)
        row_of = lax.rem(k, 2)
        v = row_of * 8 + k
        send(ea_out.at[k], ea_in.at[w], ea_send, ea_recv, (row_of, k, z, xl, core), jnp.logical_and(w < 15, w != v))
    send_a(1, windows[7:])
    ea_in[w] = ea_out[y]
    send_prior(0, w < 15)
    for q in (2, 3):
        send(x2b.at[q], rel.at[q - 2], e_send, rel_recv, at_win(jnp.int32(15)), w == 7)
    send_prior(1, w == 7)

    loads[2].wait()
    loads[3].wait()
    for t in range(4):
        rows = slice(8 * t, 8 * t + 8)
        for g in range(4):
            for q in range(4):
                at = slice(512 * g + 128 * q, 512 * g + 128 * q + 128)
                u = mb[rows, at] + later * xb[rows, at]
                lamb[rows, at] = u
                lb[rows, at] = (
                    kb[0, rows, at].astype(F32) * (ob[0, rows, at] - x1b[rows, at])
                    + kb[1, rows, at].astype(F32) * (ob[1, rows, at] - x2b[q, rows, 128 * g : 128 * g + 128])
                    + u
                )

    def piece(s):
        wait_either(w == 15, a_in.at[s, 0:15], a_in.at[s, 0:14], a_recv.at[s])
        total = jnp.zeros((8, 256), F32)
        for v in range(16):
            p_out[32 * s + v] = total[:, :128]
            p_out[32 * s + 16 + v] = total[:, 128:]
            if v < 15:
                total = total + a_in[s, v]
        for q in (2 * s, 2 * s + 1):
            for v, device in windows:
                send(p_out.at[16 * q + v], p_in.at[q, w], p_send, p_recv.at[q], device, v > 0)
            if q > 0:
                send_prior(q, jnp.logical_and(w < 15, w != 7))
        for q in (2 * s, 2 * s + 1):
            p_in[q, w] = p_out[16 * q + w]

    piece(0)

    @pl.when(holder)
    def _():
        wait_either(w == 15, ea_in.at[0:15], ea_in.at[0:14], ea_recv)
        total = jnp.zeros((8, 128), F32)
        for v in range(16):
            ep_out[v] = total
            if v < 15:
                total = total + ea_in[v]
        for v, device in windows:
            send(ep_out.at[v], ep_in.at[y], ep_send, ep_recv, device, v > 0)
        ep_in[y] = ep_out[w]

    piece(1)
    pl.when(w == 15)(relay_prior)

    for load in loads[4:]:
        load.wait()
    lsf[...] = gathered(ls[...], 32, 32) * 2.0**-22
    lnf[...] = gathered(lo[...], 16, 128)
    save_scale = pltpu.make_async_copy(lnf, lon_scale, out_sem.at[0])
    save_scale.start()

    @pl.when(w > 0)
    def _():
        wait_either(holder, ep_in.at[0:7], ep_in.at[0:8], ep_recv)

    for q in range(4):
        wait(p_in.at[q, 0:15], p_recv.at[q], w > 0)
        wait(pb.at[q], e_recv.at[q], w > 0)
        for g in range(4):
            at = slice(512 * g + 128 * q, 512 * g + 128 * q + 128)
            outer = ep_in[4 * (g % 2) + q]
            if g >= 2:
                outer = pltpu.roll(outer, 4, 0)
            for t in range(4):
                rows = slice(8 * t, 8 * t + 8)
                prior = 0.5 * pb[q, rows, 128 * g : 128 * g + 128]
                lamb[rows, at] = lamb[rows, at] - prior
                earlier = p_in[q, slot_of(t, g)]
                if t == 0:
                    earlier = jnp.where(row1 < 2, outer, earlier)
                if t == 3:
                    earlier = jnp.where(row1 >= 6, outer, earlier)
                rb[32 * g + 8 * t : 32 * g + 8 * t + 8, :] = lb[rows, at] - prior - (earlier + prior) * inv
        tb[q] = rb[...].T
        for off in AROUND:
            to = ahead(z, off)
            when = None if off else (group != q)
            device = (xh, y, to, jnp.int32(q // 2), jnp.int32(q % 2))
            send(tb.at[q, pl.ds(pl.multiple_of(to * 16, 16), 16), :], zb.at[l], z_send, z_recv, device, when)
    here = pl.ds(pl.multiple_of(z * 16, 16), 16)
    zb[l] = tb[group, here, :]
    save = pltpu.make_async_copy(lamb, new_mult, out_sem.at[1])
    save.start()

    wait(zb.at[0:31], z_recv)

    def sink(j, h, value):
        ob2[j, 8 * h : 8 * h + 8, :] = value

    operator(
        lambda j, h: zb[j, 8 * h : 8 * h + 8, :], sink, 32, 16, rows_of(twb, 0, 32), rows_of(twb, 32, 32), lsf, uv, wfb, wbb
    )
    for m, device in bands:
        send(ob2.at[m], turned.at[group, here, :], y_send, y_recv, device)
    own = pltpu.make_async_copy(ob2.at[l], turned.at[group, here, :], out_sem.at[2])
    own.start()

    wait(halo.at[0], h_send.at[0], l < 31)
    wait(halo.at[1], h_send.at[1], l > 0)

    @pl.when(w < 15)
    def _():
        wait(a_out.at[0:30], a_send)
        wait(x2b, e_send)
        wait_either(holder, ea_out.at[0:7], ea_out.at[0:8], ea_send)

    wait_either(w == 0, p_out.at[0:60], p_out.at[0:56], p_send)

    @pl.when(holder)
    def _():
        wait_either(w == 0, ep_out.at[0:15], ep_out.at[0:14], ep_send)

    wait(rel, rel_send, w == 15)
    wait(zb.at[0:31], z_send)
    save_scale.wait()
    save.wait()
    own.wait()
    wait(ob2.at[0:31], y_send)
    wait(ob2.at[0:31], y_recv)


def longitude_kernel(
    state, lam, turned, lon_scale, tw, wf, wb,
    new_state, new_mult,
    xb, lamb, yb, lnf, twb, wfb, wbb, vb, uv, outb, in_sem, out_sem,
):
    loads = [
        pltpu.make_async_copy(src, dst, in_sem.at[i])
        for i, (src, dst) in enumerate(
            [(turned, yb), (tw, twb), (wf, wfb), (lon_scale, lnf), (wb, wbb), (state, xb), (lam, lamb)]
        )
    ]
    for load in loads:
        load.start()
    loads[0].wait()
    loads[1].wait()
    for q in range(4):
        flat = yb[q].T
        for g in range(4):
            vb[4 * g + q] = flat[32 * g : 32 * g + 32, :]
    for load in loads[2:5]:
        load.wait()
    save = pltpu.make_async_copy(lamb, new_mult, out_sem.at[4])
    results = [
        pltpu.make_async_copy(outb.at[8 * h : 8 * h + 8, :], new_state.at[8 * h : 8 * h + 8, :], out_sem.at[h]) for h in range(4)
    ]

    def sink(j, h, value):
        if (j, h) == (0, 0):
            loads[5].wait()
            loads[6].wait()
            save.start()
        rows, columns = slice(8 * h, 8 * h + 8), slice(128 * j, 128 * j + 128)
        outb[rows, columns] = xb[rows, columns] + value
        if j == 15:
            results[h].start()

    operator(lambda j, h: vb[j, 8 * h : 8 * h + 8, :], sink, 16, 32, rows_of(twb, 0, 16), rows_of(twb, 16, 16), lnf, uv, wfb, wbb)
    save.wait()
    for result in results:
        result.wait()


def per_device(state, multipliers, observations, obs_mask, speed, drift, kappa, lat_spectrum, lon_spectrum):
    band, nlon = state.shape[2:]
    (tw_lat, w_lat), (tw_lon, w_lon) = tables(32, 32), tables(16, 128)
    hbm = pl.BlockSpec(memory_space=pltpu.HBM)
    vmem = pltpu.VMEM
    dma = pltpu.SemaphoreType.DMA
    grid = jax.ShapeDtypeStruct((band, nlon), F32)
    field = vmem((32, 2048), F32)
    turned, lam, lon_scale = pl.pallas_call(
        exchange_kernel,
        out_shape=[jax.ShapeDtypeStruct((4, 128, 128), F32), grid, jax.ShapeDtypeStruct((16, 128), F32)],
        in_specs=[hbm] * 4 + [pl.BlockSpec(memory_space=pltpu.SMEM)] * 3 + [hbm] * 5,
        out_specs=[hbm] * 3,
        scratch_shapes=[
            field, field, vmem((2, 32, 2048), F32), vmem((2, 32, 2048), jnp.int32),
            vmem((1, 1024), F32), vmem((1, 2048), F32), vmem((64, 128), F32), vmem((256, 256), BF16), vmem((384, 256), BF16),
            vmem((2, 8, 2048), F32), field, vmem((4, 32, 512), F32), vmem((4, 32, 512), F32), field, field,
            vmem((32, 8, 256), F32), vmem((2, 16, 8, 256), F32), vmem((64, 8, 128), F32), vmem((4, 16, 8, 128), F32),
            vmem((8, 8, 128), F32), vmem((16, 8, 128), F32), vmem((16, 8, 128), F32), vmem((8, 8, 128), F32), vmem((2, 32, 512), F32),
            vmem((128, 128), F32), vmem((4, 128, 128), F32), vmem((32, 16, 128), F32), vmem((32, 16, 128), F32),
            vmem((512, 256), F32), vmem((32, 128), F32), vmem((16, 128), F32),
            dma((9,)), dma((3,)), dma((2,)), dma((2,)), dma, dma((2,)), dma, dma((4,)),
            dma, dma, dma, dma, dma, dma((4,)), dma, dma, dma, dma, dma, dma,
        ],
        compiler_params=pltpu.CompilerParams(collective_id=0, has_side_effects=True, vmem_limit_bytes=67043328),
        name="exchange",
    )(
        state[0, 0], multipliers[0, 0], observations[0, :, 0], obs_mask[0], speed, drift, kappa, lat_spectrum, lon_spectrum,
        jnp.asarray(tw_lat), *(jnp.asarray(part) for part in weights(w_lat)),
    )
    new_state, new_mult = pl.pallas_call(
        longitude_kernel,
        out_shape=[grid] * 2,
        in_specs=[hbm] * 7,
        out_specs=[hbm] * 2,
        scratch_shapes=[
            field, field, vmem((4, 128, 128), F32), vmem((16, 128), F32), vmem((32, 128), F32),
            vmem((256, 256), BF16), vmem((384, 256), BF16), vmem((16, 32, 128), F32), vmem((512, 256), F32), field,
            dma((7,)), dma((5,)),
        ],
        compiler_params=pltpu.CompilerParams(vmem_limit_bytes=67043328),
        name="longitudes",
    )(
        state[0, 0], lam, turned, lon_scale,
        jnp.asarray(tw_lon), *(jnp.asarray(part) for part in weights(w_lon)),
    )
    return new_state[None, None], new_mult[None, None]


def solution(mesh):
    finer = Mesh(mesh.devices.reshape(2, 8, 8, 2, 2), AXES)
    placed = (
        P(WIN, None, LAT, None),
        P(WIN, None, LAT, None),
        P(WIN, None, None, LAT, None),
        P(WIN, None, LAT, None),
        P(),
        P(),
        P(),
        P(),
        P(),
    )
    return jax.shard_map(
        per_device,
        mesh=finer,
        in_specs=placed,
        out_specs=(P(WIN, None, LAT, None), P(WIN, None, LAT, None)),
        check_vma=False,
    )
```

```python
import functools
import math

import jax
import jax.numpy as jnp
import numpy as np
from jax import lax
from jax.experimental import pallas as pl
from jax.experimental.pallas import tpu as pltpu
from jax.sharding import Mesh
from jax.sharding import PartitionSpec as P

AXES = ("win_0", "win_1", "lat_0", "lat_1", "lat_2")
WIN = AXES[:2]
LAT = AXES[2:]
F32 = jnp.float32
BF16 = jnp.bfloat16
AROUND = (4, 5, 3, 6, 2, 7, 1, 0)
TILE_OF = (1, 0, 2, 3)
PARTS = 2


def rotated(c, s, angle):
    if s is None:
        return c * math.cos(angle), c * math.sin(angle)
    cos, sin = math.cos(angle), math.sin(angle)
    return c * cos - s * sin, c * sin + s * cos


def rfft(xs):
    n = len(xs)
    if n == 2:
        return [(xs[0] + xs[1], None), (xs[0] - xs[1], None)]
    even, odd = rfft(xs[0::2]), rfft(xs[1::2])
    out = [None] * (n // 2 + 1)
    for k in range(n // 4 + 1):
        (ec, es), (oc, os) = even[k], odd[k]
        if k == 0:
            out[0] = (ec + oc, None)
            out[n // 2] = (ec - oc, None)
        elif k == n // 4:
            out[k] = (ec, oc)
        else:
            tc, ts = rotated(oc, os, 2 * math.pi * k / n)
            if es is None:
                out[k] = (ec + tc, ts)
                out[n // 2 - k] = (ec - tc, ts)
            else:
                out[k] = (ec + tc, es + ts)
                out[n // 2 - k] = (ec - tc, ts - es)
    return out


def synth(n, c, s):
    if n == 2:
        return [c[0] + c[1], c[0] - c[1]]
    half, quarter = n // 2, n // 4
    ec, es, oc, os = [], [], [], []
    for k in range(quarter + 1):
        if k == quarter:
            ec.append(c[k])
            es.append(None)
            oc.append(s[k])
            os.append(None)
        elif k == 0:
            ec.append(c[0] + c[half])
            es.append(None)
            oc.append(c[0] - c[half])
            os.append(None)
        else:
            cos, sin = math.cos(2 * math.pi * k / n), math.sin(2 * math.pi * k / n)
            ec.append(c[k] + c[half - k])
            es.append(s[k] - s[half - k])
            dc, ds = c[k] - c[half - k], s[k] + s[half - k]
            oc.append(dc * cos + ds * sin)
            os.append(ds * cos - dc * sin)
    out = [None] * n
    out[0::2] = synth(half, ec, es)
    out[1::2] = synth(half, oc, os)
    return out


def analyse(xs, cos, sin):
    n = len(xs)
    bins = rfft(xs)
    u, v = [], []
    for k in range(n):
        c, s = bins[k] if k <= n // 2 else bins[n - k]
        if k == 0:
            u.append(c)
            v.append(c * 0.0)
        elif s is None:
            u.append(c * cos[k])
            v.append(c * sin[k])
        elif k <= n // 2:
            u.append(c * cos[k] - s * sin[k])
            v.append(c * sin[k] + s * cos[k])
        else:
            u.append(c * cos[k] + s * sin[k])
            v.append(c * sin[k] - s * cos[k])
    return u, v


def synthesise(u, v, cos, sin):
    n = len(u)
    c, s = [u[0]], [None]
    for k in range(1, n):
        c.append(u[k] * cos[k] + v[k] * sin[k])
        s.append(None if k == n // 2 else v[k] * cos[k] - u[k] * sin[k])
    half = n // 2
    fc = [c[0]] + [c[k] + c[n - k] for k in range(1, half)] + [c[half]]
    fs = [None] + [s[k] - s[n - k] for k in range(1, half)] + [None]
    return synth(n, fc, fs)


def twiddle(n1, n2):
    angle = 2 * np.pi * np.arange(n1)[:, None] * np.arange(n2)[None] / (n1 * n2)
    return np.cos(angle), np.sin(angle)


def casmat(n2):
    angle = 2 * np.pi * (np.arange(n2)[:, None] * np.arange(n2)[None] % n2) / n2
    cos, sin = np.cos(angle), np.sin(angle)
    return np.concatenate([cos + sin, cos - sin], 0)


def tables(n1, n2):
    copies = 128 // n2
    cos, sin = (np.tile(t, (1, copies)) for t in twiddle(n1, n2))
    one = casmat(n2)
    eye = np.eye(copies)
    full = np.concatenate([np.kron(eye, one[:n2]), np.kron(eye, one[n2:])], 0)
    return np.concatenate([cos, sin], 0).astype(np.float32), full.astype(np.float32)


def weights(full):
    import ml_dtypes

    first = full.astype(ml_dtypes.bfloat16)
    rest = (full - first.astype(np.float32)).astype(ml_dtypes.bfloat16)
    return np.concatenate([first, rest], 1), np.ascontiguousarray(np.concatenate([first.T, first.T, rest.T], 0))


def parted(a):
    first = a.astype(BF16)
    return first, (a - first.astype(F32)).astype(BF16)


def dot(a, b):
    return jnp.dot(a, b, preferred_element_type=F32)


def gathered(spec, n1, n2):
    n = n1 * n2
    rows = lax.broadcasted_iota(jnp.int32, (n1, n), 0)
    lanes = lax.broadcasted_iota(jnp.int32, (n1, n), 1)
    own = jnp.where((lanes & (n1 - 1)) == rows, jnp.broadcast_to(spec, (n1, n)), 0.0)
    first = own.astype(BF16)
    rest = own - first.astype(F32)
    second = rest.astype(BF16)
    third = (rest - second.astype(F32)).astype(BF16)
    place = lax.broadcasted_iota(jnp.int32, (n, 128), 0) >> (n1.bit_length() - 1)
    lane = lax.broadcasted_iota(jnp.int32, (n, 128), 1) & (n2 - 1)
    pick = jnp.where(place == lane, 1.0, 0.0).astype(BF16)
    return dot(first, pick) + dot(second, pick) + dot(third, pick)


def slot_of(tile, group):
    return (group // 2) * 8 + (group % 2) * 4 + TILE_OF.index(tile)


def operator(source, sink, n1, depth, cos, sin, scale, uv, wf, wb):
    for h in range(depth // 8):
        u, v = analyse([source(j, h) for j in range(n1)], cos, sin)
        for k in range(n1):
            at = depth * k + 8 * h
            uv[at : at + 8, 0:128] = u[k]
            uv[at : at + 8, 128:256] = v[k]
    count = 512 // PARTS
    for q in range(PARTS):
        rows = slice(count * q, count * (q + 1))
        factor = jnp.concatenate(
            [jnp.broadcast_to(scale[k : k + 1, :], (depth, 128)) for k in range(count * q // depth, count * (q + 1) // depth)],
            axis=0,
        )
        first, rest = parted(uv[rows, :])
        both = dot(first, wf[...])
        spectral = (both[:, :128] + (both[:, 128:] + dot(rest, wf[:, 0:128]))) * factor
        first, rest = parted(spectral)
        uv[rows, :] = dot(jnp.concatenate([first, rest], axis=1), wb[0:256, :]) + dot(first, wb[256:384, :])
    for h in range(depth // 8):
        at = [depth * k + 8 * h for k in range(n1)]
        out = synthesise([uv[a : a + 8, 0:128] for a in at], [uv[a : a + 8, 128:256] for a in at], cos, sin)
        for j in range(n1):
            sink(j, h, out[j])


def rows_of(ref, first, count):
    return [ref[first + k : first + k + 1, :] for k in range(count)]


def exchange_kernel(
    state, mult, obs, mask, speed, drift, kappa, lat_spec, lon_spec, tw, wf, wb,
    turned, new_mult, lon_scale,
    xb, mb, ob, kb, ls, lo, twb, wfb, wbb,
    halo, x1b, x2b, pb, lb, lamb, a_out, a_in, p0_out, p0_in, p_out, p_in, ea_out, ea_in, ep_out, ep_in, rel,
    rb, tb, zb, ob2, uv, lsf, lnf,
    in_sem, out_sem, h_send, h_recv, a_send, a_recv, p_send, p_recv, ea_send, ea_recv, ep_send, ep_recv,
    e_send, e_recv, rel_send, rel_recv, z_send, z_recv, y_send, y_recv,
):
    xh, y, z, xl, core = (lax.axis_index(a) for a in AXES)
    w = xh * 8 + y
    l = z * 4 + xl * 2 + core
    group = xl * 2 + core

    def at_win(v):
        return (lax.div(v, 8), lax.rem(v, 8), z, xl, core)

    def at_lat(m):
        return (xh, y, lax.div(m, 4), lax.rem(lax.div(m, 2), 2), lax.rem(m, 2))

    loads = [
        pltpu.make_async_copy(src, dst, in_sem.at[i])
        for i, (src, dst) in enumerate(
            [(state, xb), (mult, mb), (obs, ob), (mask, kb), (lat_spec, ls), (lon_spec, lo), (tw, twb), (wf, wfb), (wb, wbb)]
        )
    ]
    for load in loads:
        load.start()

    def ahead(place, off):
        return jnp.where(place + off >= 8, place + off - 8, place + off) if off else place

    windows, bands = [], []
    for off in AROUND:
        yy, zz = ahead(y, off), ahead(z, off)
        for xx in (1 - xh, xh):
            if off or xx is not xh:
                windows.append((xx * 8 + yy, (xx, yy, z, xl, core)))
        for xx, cc in ((1 - xl, core), (1 - xl, 1 - core), (xl, 1 - core), (xl, core)):
            if off or xx is not xl or cc is not core:
                bands.append((zz * 4 + xx * 2 + cc, (xh, y, zz, xx, cc)))
    barrier = pltpu.get_barrier_semaphore()
    for _, device in windows + bands:
        pl.semaphore_signal(barrier, inc=1, device_id=device, device_id_type=pl.DeviceIdType.MESH)

    def guarded(when, act):
        if when is None:
            act()
        else:
            pl.when(when)(act)

    def send(src, dst, send_sem, recv_sem, device, when=None):
        copy = pltpu.make_async_remote_copy(
            src_ref=src, dst_ref=dst, send_sem=send_sem, recv_sem=recv_sem,
            device_id=device, device_id_type=pl.DeviceIdType.MESH,
        )
        guarded(when, copy.start)

    def wait(like, sem, when=None):
        guarded(when, pltpu.make_async_copy(like, like, sem).wait)

    def wait_either(when, first, second, sem):
        wait(first, sem, when)
        wait(second, sem, jnp.logical_not(when))

    row = lax.broadcasted_iota(jnp.int32, (8, 2048), 0)
    row8 = lax.broadcasted_iota(jnp.int32, (8, 1024), 0)
    row1 = lax.broadcasted_iota(jnp.int32, (8, 128), 0)
    later = jnp.where(w > 0, F32(0.5), F32(0.0))
    inv = F32(1.0)
    for k in range(2, 16):
        inv = jnp.where(w == k, F32(1.0 / k), inv)
    sp, dr, ka = speed[0], drift[0], kappa[0]

    def step(mid, north, south):
        east = pltpu.roll(mid, 2047, 1)
        west = pltpu.roll(mid, 1, 1)
        return (
            mid
            - (sp * mid * (east - west)) * 0.5
            - (dr * (north - south)) * 0.5
            + ka * (east + west + north + south - 4.0 * mid)
        )

    def advanced(before, mid, after):
        north, south = pltpu.roll(mid, 7, 0), pltpu.roll(mid, 1, 0)
        if after is not None:
            north = jnp.where(row == 7, pltpu.roll(after, 7, 0), north)
        if before is not None:
            south = jnp.where(row == 0, pltpu.roll(before, 1, 0), south)
        return step(mid, north, south)

    def tile(ref, t):
        return ref[8 * t : 8 * t + 8, :]

    def keep(t, second):
        for g in range(4):
            for q in range(4):
                at = 512 * g + 128 * q
                x2b[q, 8 * t : 8 * t + 8, 128 * g : 128 * g + 128] = second[:, at : at + 128]

    def term(t, second):
        return tile(mb, t) + later * tile(xb, t) - 0.5 * second

    def send_prior(q, when):
        send(x2b.at[q], pb.at[q], e_send, e_recv.at[q], at_win(lax.rem(w + 1, 16)), when)

    def relay_prior():
        wait(rel, rel_recv)
        for q in (2, 3):
            send(rel.at[q - 2], pb.at[q], rel_send, e_recv.at[q], at_win(jnp.int32(8)))

    loads[0].wait()
    first = [tile(xb, t) for t in range(4)]
    for t in range(4):
        x1b[8 * t : 8 * t + 8, :] = advanced(
            first[t - 1] if t > 0 else None, first[t], first[t + 1] if t < 3 else None
        )
    loads[1].wait()
    for t in range(4):
        second = advanced(
            tile(x1b, t - 1) if t > 0 else None, tile(x1b, t), tile(x1b, t + 1) if t < 3 else None
        )
        if t in (1, 2):
            keep(t, second)
        a = term(t, second)
        for g in range(4):
            for s in range(2):
                a_out[16 * s + slot_of(t, g)] = a[:, 512 * g + 256 * s : 512 * g + 256 * s + 256]
    pl.semaphore_wait(barrier, 46)
    north_of, south_of = lax.rem(l + 1, 32), lax.rem(l + 31, 32)
    send(xb.at[24:32, :], halo.at[0], h_send.at[0], h_recv.at[0], at_lat(north_of), l < 31)
    send(xb.at[0:8, :], halo.at[1], h_send.at[1], h_recv.at[1], at_lat(south_of), l > 0)

    def send_a(s, some):
        for v, device in some:
            send(a_out.at[16 * s + v], a_in.at[s, w], a_send, a_recv.at[s], device, w < 15)

    send_a(0, windows)
    send_a(1, windows[:7])
    for s in range(2):
        a_in[s, w] = a_out[16 * s + w]

    @pl.when(l == 0)
    def _():
        halo[0] = jnp.zeros((8, 2048), F32)

    @pl.when(l == 31)
    def _():
        halo[1] = jnp.zeros((8, 2048), F32)

    @pl.when(w == 0)
    def _():
        pb[...] = jnp.zeros(pb.shape, F32)
        p0_in[...] = jnp.zeros(p0_in.shape, F32)
        p_in[...] = jnp.zeros(p_in.shape, F32)
        ep_in[...] = jnp.zeros(ep_in.shape, F32)

    wait(halo.at[0], h_recv.at[0], l > 0)
    wait(halo.at[1], h_recv.at[1], l < 31)
    low, high = halo[0], halo[1]
    beyond_low = jnp.where(l > 0, advanced(None, low, tile(xb, 0)), 0.0)
    edge = advanced(low, tile(xb, 0), tile(xb, 1))
    x1b[0:8, :] = edge
    bottom = advanced(beyond_low, edge, tile(x1b, 1))
    beyond_high = jnp.where(l < 31, advanced(tile(xb, 3), high, None), 0.0)
    edge = advanced(tile(xb, 2), tile(xb, 3), high)
    x1b[24:32, :] = edge
    top = advanced(tile(x1b, 2), edge, beyond_high)
    keep(0, bottom)
    keep(3, top)
    outer = jnp.where(row < 4, term(0, bottom), term(3, top))
    packed = jnp.where((row8 < 2) | (row8 >= 6), outer[:, :1024], pltpu.roll(outer[:, 1024:], 4, 0))
    holder = lax.rem(y, 2) == xh
    for k in range(8):
        ea_out[k] = packed[:, 128 * k : 128 * k + 128]
    for off in AROUND:
        k = ahead(y, off)
        row_of = lax.rem(k, 2)
        v = row_of * 8 + k
        send(ea_out.at[k], ea_in.at[w], ea_send, ea_recv, (row_of, k, z, xl, core), jnp.logical_and(w < 15, w != v))
    send_a(1, windows[7:])
    ea_in[w] = ea_out[y]
    send_prior(0, w < 15)
    for q in (2, 3):
        send(x2b.at[q], rel.at[q - 2], e_send, rel_recv, at_win(jnp.int32(15)), w == 7)
    send_prior(1, w == 7)

    loads[2].wait()
    loads[3].wait()
    for t in range(4):
        rows = slice(8 * t, 8 * t + 8)
        for g in range(4):
            for q in range(4):
                at = slice(512 * g + 128 * q, 512 * g + 128 * q + 128)
                u = mb[rows, at] + later * xb[rows, at]
                lamb[rows, at] = u
                lb[rows, at] = (
                    kb[0, rows, at].astype(F32) * (ob[0, rows, at] - x1b[rows, at])
                    + kb[1, rows, at].astype(F32) * (ob[1, rows, at] - x2b[q, rows, 128 * g : 128 * g + 128])
                    + u
                )

    def piece(s):
        wait_either(w == 15, a_in.at[s, 0:15], a_in.at[s, 0:14], a_recv.at[s])
        total = jnp.zeros((8, 256), F32)
        for v in range(16):
            if s == 0:
                p0_out[v] = total
            else:
                p_out[v] = total[:, :128]
                p_out[16 + v] = total[:, 128:]
            if v < 15:
                total = total + a_in[s, v]
        if s == 0:
            for v, device in windows:
                send(p0_out.at[v], p0_in.at[w], p_send, p_recv.at[0], device, v > 0)
            send_prior(1, jnp.logical_and(w < 15, w != 7))
            p0_in[w] = p0_out[w]
            return
        for q in range(2):
            for v, device in windows:
                send(p_out.at[16 * q + v], p_in.at[q, w], p_send, p_recv.at[1 + q], device, v > 0)
            send_prior(2 + q, jnp.logical_and(w < 15, w != 7))
        for q in range(2):
            p_in[q, w] = p_out[16 * q + w]

    piece(0)

    @pl.when(holder)
    def _():
        wait_either(w == 15, ea_in.at[0:15], ea_in.at[0:14], ea_recv)
        total = jnp.zeros((8, 128), F32)
        for v in range(16):
            ep_out[v] = total
            if v < 15:
                total = total + ea_in[v]
        for v, device in windows:
            send(ep_out.at[v], ep_in.at[y], ep_send, ep_recv, device, v > 0)
        ep_in[y] = ep_out[w]

    piece(1)
    pl.when(w == 15)(relay_prior)

    for load in loads[4:]:
        load.wait()
    lsf[...] = gathered(ls[...], 32, 32) * 2.0**-22
    lnf[...] = gathered(lo[...], 16, 128)
    save_scale = pltpu.make_async_copy(lnf, lon_scale, out_sem.at[0])
    save_scale.start()

    @pl.when(w > 0)
    def _():
        wait_either(holder, ep_in.at[0:7], ep_in.at[0:8], ep_recv)

    for q in range(4):
        if q == 0:
            wait(p0_in.at[0:15], p_recv.at[0], w > 0)
        if q >= 2:
            wait(p_in.at[q - 2, 0:15], p_recv.at[q - 1], w > 0)
        wait(pb.at[q], e_recv.at[q], w > 0)
        for g in range(4):
            at = slice(512 * g + 128 * q, 512 * g + 128 * q + 128)
            outer = ep_in[4 * (g % 2) + q]
            if g >= 2:
                outer = pltpu.roll(outer, 4, 0)
            for t in range(4):
                rows = slice(8 * t, 8 * t + 8)
                prior = 0.5 * pb[q, rows, 128 * g : 128 * g + 128]
                lamb[rows, at] = lamb[rows, at] - prior
                if q < 2:
                    earlier = p0_in[slot_of(t, g), :, 128 * q : 128 * q + 128]
                else:
                    earlier = p_in[q - 2, slot_of(t, g)]
                if t == 0:
                    earlier = jnp.where(row1 < 2, outer, earlier)
                if t == 3:
                    earlier = jnp.where(row1 >= 6, outer, earlier)
                rb[32 * g + 8 * t : 32 * g + 8 * t + 8, :] = lb[rows, at] - prior - (earlier + prior) * inv
        tb[q] = rb[...].T
        for off in AROUND:
            to = ahead(z, off)
            when = None if off else (group != q)
            device = (xh, y, to, jnp.int32(q // 2), jnp.int32(q % 2))
            send(tb.at[q, pl.ds(pl.multiple_of(to * 16, 16), 16), :], zb.at[l], z_send, z_recv, device, when)
    here = pl.ds(pl.multiple_of(z * 16, 16), 16)
    zb[l] = tb[group, here, :]
    save = pltpu.make_async_copy(lamb, new_mult, out_sem.at[1])
    save.start()

    wait(zb.at[0:31], z_recv)

    def sink(j, h, value):
        ob2[j, 8 * h : 8 * h + 8, :] = value

    operator(
        lambda j, h: zb[j, 8 * h : 8 * h + 8, :], sink, 32, 16, rows_of(twb, 0, 32), rows_of(twb, 32, 32), lsf, uv, wfb, wbb
    )
    for m, device in bands:
        send(ob2.at[m], turned.at[group, here, :], y_send, y_recv, device)
    own = pltpu.make_async_copy(ob2.at[l], turned.at[group, here, :], out_sem.at[2])
    own.start()

    wait(halo.at[0], h_send.at[0], l < 31)
    wait(halo.at[1], h_send.at[1], l > 0)

    @pl.when(w < 15)
    def _():
        wait(a_out.at[0:30], a_send)
        wait(x2b, e_send)
        wait_either(holder, ea_out.at[0:7], ea_out.at[0:8], ea_send)

    wait_either(w == 0, a_out.at[0:30], a_out.at[0:28], p_send)

    @pl.when(holder)
    def _():
        wait_either(w == 0, ep_out.at[0:15], ep_out.at[0:14], ep_send)

    wait(rel, rel_send, w == 15)
    wait(zb.at[0:31], z_send)
    save_scale.wait()
    save.wait()
    own.wait()
    wait(ob2.at[0:31], y_send)
    wait(ob2.at[0:31], y_recv)


def longitude_kernel(
    state, lam, turned, lon_scale, tw, wf, wb,
    new_state, new_mult,
    xb, lamb, yb, lnf, twb, wfb, wbb, vb, uv, outb, in_sem, out_sem,
):
    loads = [
        pltpu.make_async_copy(src, dst, in_sem.at[i])
        for i, (src, dst) in enumerate(
            [(turned, yb), (tw, twb), (wf, wfb), (lon_scale, lnf), (wb, wbb), (state, xb), (lam, lamb)]
        )
    ]
    for load in loads:
        load.start()
    loads[0].wait()
    loads[1].wait()
    for q in range(4):
        flat = yb[q].T
        for g in range(4):
            vb[4 * g + q] = flat[32 * g : 32 * g + 32, :]
    for load in loads[2:5]:
        load.wait()
    save = pltpu.make_async_copy(lamb, new_mult, out_sem.at[4])
    results = [
        pltpu.make_async_copy(outb.at[8 * h : 8 * h + 8, :], new_state.at[8 * h : 8 * h + 8, :], out_sem.at[h]) for h in range(4)
    ]

    def sink(j, h, value):
        if (j, h) == (0, 0):
            loads[5].wait()
            loads[6].wait()
            save.start()
        rows, columns = slice(8 * h, 8 * h + 8), slice(128 * j, 128 * j + 128)
        outb[rows, columns] = xb[rows, columns] + value
        if j == 15:
            results[h].start()

    operator(lambda j, h: vb[j, 8 * h : 8 * h + 8, :], sink, 16, 32, rows_of(twb, 0, 16), rows_of(twb, 16, 16), lnf, uv, wfb, wbb)
    save.wait()
    for result in results:
        result.wait()


def per_device(state, multipliers, observations, obs_mask, speed, drift, kappa, lat_spectrum, lon_spectrum):
    band, nlon = state.shape[2:]
    (tw_lat, w_lat), (tw_lon, w_lon) = tables(32, 32), tables(16, 128)
    hbm = pl.BlockSpec(memory_space=pltpu.HBM)
    vmem = pltpu.VMEM
    dma = pltpu.SemaphoreType.DMA
    grid = jax.ShapeDtypeStruct((band, nlon), F32)
    field = vmem((32, 2048), F32)
    turned, lam, lon_scale = pl.pallas_call(
        exchange_kernel,
        out_shape=[jax.ShapeDtypeStruct((4, 128, 128), F32), grid, jax.ShapeDtypeStruct((16, 128), F32)],
        in_specs=[hbm] * 4 + [pl.BlockSpec(memory_space=pltpu.SMEM)] * 3 + [hbm] * 5,
        out_specs=[hbm] * 3,
        scratch_shapes=[
            field, field, vmem((2, 32, 2048), F32), vmem((2, 32, 2048), jnp.int32),
            vmem((1, 1024), F32), vmem((1, 2048), F32), vmem((64, 128), F32), vmem((256, 256), BF16), vmem((384, 256), BF16),
            vmem((2, 8, 2048), F32), field, vmem((4, 32, 512), F32), vmem((4, 32, 512), F32), field, field,
            vmem((32, 8, 256), F32), vmem((2, 16, 8, 256), F32), vmem((16, 8, 256), F32), vmem((16, 8, 256), F32),
            vmem((32, 8, 128), F32), vmem((2, 16, 8, 128), F32),
            vmem((8, 8, 128), F32), vmem((16, 8, 128), F32), vmem((16, 8, 128), F32), vmem((8, 8, 128), F32), vmem((2, 32, 512), F32),
            vmem((128, 128), F32), vmem((4, 128, 128), F32), vmem((32, 16, 128), F32), vmem((32, 16, 128), F32),
            vmem((512, 256), F32), vmem((32, 128), F32), vmem((16, 128), F32),
            dma((9,)), dma((3,)), dma((2,)), dma((2,)), dma, dma((2,)), dma, dma((3,)),
            dma, dma, dma, dma, dma, dma((4,)), dma, dma, dma, dma, dma, dma,
        ],
        compiler_params=pltpu.CompilerParams(collective_id=0, has_side_effects=True, vmem_limit_bytes=67043328),
        name="exchange",
    )(
        state[0, 0], multipliers[0, 0], observations[0, :, 0], obs_mask[0], speed, drift, kappa, lat_spectrum, lon_spectrum,
        jnp.asarray(tw_lat), *(jnp.asarray(part) for part in weights(w_lat)),
    )
    new_state, new_mult = pl.pallas_call(
        longitude_kernel,
        out_shape=[grid] * 2,
        in_specs=[hbm] * 7,
        out_specs=[hbm] * 2,
        scratch_shapes=[
            field, field, vmem((4, 128, 128), F32), vmem((16, 128), F32), vmem((32, 128), F32),
            vmem((256, 256), BF16), vmem((384, 256), BF16), vmem((16, 32, 128), F32), vmem((512, 256), F32), field,
            dma((7,)), dma((5,)),
        ],
        compiler_params=pltpu.CompilerParams(vmem_limit_bytes=67043328),
        name="longitudes",
    )(
        state[0, 0], lam, turned, lon_scale,
        jnp.asarray(tw_lon), *(jnp.asarray(part) for part in weights(w_lon)),
    )
    return new_state[None, None], new_mult[None, None]


def solution(mesh):
    finer = Mesh(mesh.devices.reshape(2, 8, 8, 2, 2), AXES)
    placed = (
        P(WIN, None, LAT, None),
        P(WIN, None, LAT, None),
        P(WIN, None, None, LAT, None),
        P(WIN, None, LAT, None),
        P(),
        P(),
        P(),
        P(),
        P(),
    )
    return jax.shard_map(
        per_device,
        mesh=finer,
        in_specs=placed,
        out_specs=(P(WIN, None, LAT, None), P(WIN, None, LAT, None)),
        check_vma=False,
    )
```

```python
import functools
import math

import jax
import jax.numpy as jnp
import numpy as np
from jax import lax
from jax.experimental import pallas as pl
from jax.experimental.pallas import tpu as pltpu
from jax.sharding import Mesh
from jax.sharding import PartitionSpec as P

AXES = ("win_0", "win_1", "lat_0", "lat_1", "lat_2")
WIN = AXES[:2]
LAT = AXES[2:]
F32 = jnp.float32
BF16 = jnp.bfloat16
AROUND = (4, 5, 3, 6, 2, 7, 1, 0)
TILE_OF = (1, 0, 2, 3)
PARTS = 4


def rotated(c, s, angle):
    if s is None:
        return c * math.cos(angle), c * math.sin(angle)
    cos, sin = math.cos(angle), math.sin(angle)
    return c * cos - s * sin, c * sin + s * cos


def rfft(xs):
    n = len(xs)
    if n == 2:
        return [(xs[0] + xs[1], None), (xs[0] - xs[1], None)]
    even, odd = rfft(xs[0::2]), rfft(xs[1::2])
    out = [None] * (n // 2 + 1)
    for k in range(n // 4 + 1):
        (ec, es), (oc, os) = even[k], odd[k]
        if k == 0:
            out[0] = (ec + oc, None)
            out[n // 2] = (ec - oc, None)
        elif k == n // 4:
            out[k] = (ec, oc)
        else:
            tc, ts = rotated(oc, os, 2 * math.pi * k / n)
            if es is None:
                out[k] = (ec + tc, ts)
                out[n // 2 - k] = (ec - tc, ts)
            else:
                out[k] = (ec + tc, es + ts)
                out[n // 2 - k] = (ec - tc, ts - es)
    return out


def synth(n, c, s):
    if n == 2:
        return [c[0] + c[1], c[0] - c[1]]
    half, quarter = n // 2, n // 4
    ec, es, oc, os = [], [], [], []
    for k in range(quarter + 1):
        if k == quarter:
            ec.append(c[k])
            es.append(None)
            oc.append(s[k])
            os.append(None)
        elif k == 0:
            ec.append(c[0] + c[half])
            es.append(None)
            oc.append(c[0] - c[half])
            os.append(None)
        else:
            cos, sin = math.cos(2 * math.pi * k / n), math.sin(2 * math.pi * k / n)
            ec.append(c[k] + c[half - k])
            es.append(s[k] - s[half - k])
            dc, ds = c[k] - c[half - k], s[k] + s[half - k]
            oc.append(dc * cos + ds * sin)
            os.append(ds * cos - dc * sin)
    out = [None] * n
    out[0::2] = synth(half, ec, es)
    out[1::2] = synth(half, oc, os)
    return out


def analyse(xs, cos, sin):
    n = len(xs)
    bins = rfft(xs)
    u, v = [], []
    for k in range(n):
        c, s = bins[k] if k <= n // 2 else bins[n - k]
        if k == 0:
            u.append(c)
            v.append(c * 0.0)
        elif s is None:
            u.append(c * cos[k])
            v.append(c * sin[k])
        elif k <= n // 2:
            u.append(c * cos[k] - s * sin[k])
            v.append(c * sin[k] + s * cos[k])
        else:
            u.append(c * cos[k] + s * sin[k])
            v.append(c * sin[k] - s * cos[k])
    return u, v


def synthesise(u, v, cos, sin):
    n = len(u)
    c, s = [u[0]], [None]
    for k in range(1, n):
        c.append(u[k] * cos[k] + v[k] * sin[k])
        s.append(None if k == n // 2 else v[k] * cos[k] - u[k] * sin[k])
    half = n // 2
    fc = [c[0]] + [c[k] + c[n - k] for k in range(1, half)] + [c[half]]
    fs = [None] + [s[k] - s[n - k] for k in range(1, half)] + [None]
    return synth(n, fc, fs)


def twiddle(n1, n2):
    angle = 2 * np.pi * np.arange(n1)[:, None] * np.arange(n2)[None] / (n1 * n2)
    return np.cos(angle), np.sin(angle)


def casmat(n2):
    angle = 2 * np.pi * (np.arange(n2)[:, None] * np.arange(n2)[None] % n2) / n2
    cos, sin = np.cos(angle), np.sin(angle)
    return np.concatenate([cos + sin, cos - sin], 0)


def tables(n1, n2):
    copies = 128 // n2
    cos, sin = (np.tile(t, (1, copies)) for t in twiddle(n1, n2))
    one = casmat(n2)
    eye = np.eye(copies)
    full = np.concatenate([np.kron(eye, one[:n2]), np.kron(eye, one[n2:])], 0)
    return np.concatenate([cos, sin], 0).astype(np.float32), full.astype(np.float32)


def weights(full):
    import ml_dtypes

    first = full.astype(ml_dtypes.bfloat16)
    rest = (full - first.astype(np.float32)).astype(ml_dtypes.bfloat16)
    return np.concatenate([first, rest], 1), np.ascontiguousarray(np.concatenate([first.T, first.T, rest.T], 0))


def parted(a):
    first = a.astype(BF16)
    return first, (a - first.astype(F32)).astype(BF16)


def dot(a, b):
    return jnp.dot(a, b, preferred_element_type=F32)


def gathered(spec, n1, n2):
    n = n1 * n2
    rows = lax.broadcasted_iota(jnp.int32, (n1, n), 0)
    lanes = lax.broadcasted_iota(jnp.int32, (n1, n), 1)
    own = jnp.where((lanes & (n1 - 1)) == rows, jnp.broadcast_to(spec, (n1, n)), 0.0)
    first = own.astype(BF16)
    rest = own - first.astype(F32)
    second = rest.astype(BF16)
    third = (rest - second.astype(F32)).astype(BF16)
    place = lax.broadcasted_iota(jnp.int32, (n, 128), 0) >> (n1.bit_length() - 1)
    lane = lax.broadcasted_iota(jnp.int32, (n, 128), 1) & (n2 - 1)
    pick = jnp.where(place == lane, 1.0, 0.0).astype(BF16)
    return dot(first, pick) + dot(second, pick) + dot(third, pick)


def slot_of(tile, group):
    return (group // 2) * 8 + (group % 2) * 4 + TILE_OF.index(tile)


def operator(source, sink, n1, depth, cos, sin, scale, uv, wf, wb):
    for h in range(depth // 8):
        u, v = analyse([source(j, h) for j in range(n1)], cos, sin)
        for k in range(n1):
            at = depth * k + 8 * h
            uv[at : at + 8, 0:128] = u[k]
            uv[at : at + 8, 128:256] = v[k]
    count = 512 // PARTS
    for q in range(PARTS):
        rows = slice(count * q, count * (q + 1))
        factor = jnp.concatenate(
            [jnp.broadcast_to(scale[k : k + 1, :], (depth, 128)) for k in range(count * q // depth, count * (q + 1) // depth)],
            axis=0,
        )
        first, rest = parted(uv[rows, :])
        both = dot(first, wf[...])
        spectral = (both[:, :128] + (both[:, 128:] + dot(rest, wf[:, 0:128]))) * factor
        first, rest = parted(spectral)
        uv[rows, :] = dot(jnp.concatenate([first, rest], axis=1), wb[0:256, :]) + dot(first, wb[256:384, :])
    for h in range(depth // 8):
        at = [depth * k + 8 * h for k in range(n1)]
        out = synthesise([uv[a : a + 8, 0:128] for a in at], [uv[a : a + 8, 128:256] for a in at], cos, sin)
        for j in range(n1):
            sink(j, h, out[j])


def rows_of(ref, first, count):
    return [ref[first + k : first + k + 1, :] for k in range(count)]


def exchange_kernel(
    state, mult, obs, mask, speed, drift, kappa, lat_spec, lon_spec, tw, wf, wb,
    turned, new_mult, lon_scale,
    xb, mb, ob, kb, ls, lo, twb, wfb, wbb,
    halo, x1b, x2b, pb, lb, lamb, a_out, a_in, p_out, p_in, ea_out, ea_in, ep_out, ep_in, rel,
    rb, tb, zb, ob2, uv, lsf, lnf,
    in_sem, out_sem, h_send, h_recv, a_send, a_recv, p_send, p_recv, ea_send, ea_recv, ep_send, ep_recv,
    e_send, e_recv, rel_send, rel_recv, z_send, z_recv, y_send, y_recv,
):
    xh, y, z, xl, core = (lax.axis_index(a) for a in AXES)
    w = xh * 8 + y
    l = z * 4 + xl * 2 + core
    group = xl * 2 + core

    def at_win(v):
        return (lax.div(v, 8), lax.rem(v, 8), z, xl, core)

    def at_lat(m):
        return (xh, y, lax.div(m, 4), lax.rem(lax.div(m, 2), 2), lax.rem(m, 2))

    loads = [
        pltpu.make_async_copy(src, dst, in_sem.at[i])
        for i, (src, dst) in enumerate(
            [(state, xb), (mult, mb), (obs, ob), (mask, kb), (lat_spec, ls), (lon_spec, lo), (tw, twb), (wf, wfb), (wb, wbb)]
        )
    ]
    for load in loads:
        load.start()

    def ahead(place, off):
        return jnp.where(place + off >= 8, place + off - 8, place + off) if off else place

    windows, bands = [], []
    for off in AROUND:
        yy, zz = ahead(y, off), ahead(z, off)
        for xx in (1 - xh, xh):
            if off or xx is not xh:
                windows.append((xx * 8 + yy, (xx, yy, z, xl, core)))
        for xx, cc in ((1 - xl, core), (1 - xl, 1 - core), (xl, 1 - core), (xl, core)):
            if off or xx is not xl or cc is not core:
                bands.append((zz * 4 + xx * 2 + cc, (xh, y, zz, xx, cc)))
    barrier = pltpu.get_barrier_semaphore()
    for _, device in windows + bands:
        pl.semaphore_signal(barrier, inc=1, device_id=device, device_id_type=pl.DeviceIdType.MESH)

    def guarded(when, act):
        if when is None:
            act()
        else:
            pl.when(when)(act)

    def send(src, dst, send_sem, recv_sem, device, when=None):
        copy = pltpu.make_async_remote_copy(
            src_ref=src, dst_ref=dst, send_sem=send_sem, recv_sem=recv_sem,
            device_id=device, device_id_type=pl.DeviceIdType.MESH,
        )
        guarded(when, copy.start)

    def wait(like, sem, when=None):
        guarded(when, pltpu.make_async_copy(like, like, sem).wait)

    def wait_either(when, first, second, sem):
        wait(first, sem, when)
        wait(second, sem, jnp.logical_not(when))

    row = lax.broadcasted_iota(jnp.int32, (8, 2048), 0)
    row8 = lax.broadcasted_iota(jnp.int32, (8, 1024), 0)
    row1 = lax.broadcasted_iota(jnp.int32, (8, 128), 0)
    later = jnp.where(w > 0, F32(0.5), F32(0.0))
    inv = F32(1.0)
    for k in range(2, 16):
        inv = jnp.where(w == k, F32(1.0 / k), inv)
    sp, dr, ka = speed[0], drift[0], kappa[0]

    def step(mid, north, south):
        east = pltpu.roll(mid, 2047, 1)
        west = pltpu.roll(mid, 1, 1)
        return (
            mid
            - (sp * mid * (east - west)) * 0.5
            - (dr * (north - south)) * 0.5
            + ka * (east + west + north + south - 4.0 * mid)
        )

    def advanced(before, mid, after):
        north, south = pltpu.roll(mid, 7, 0), pltpu.roll(mid, 1, 0)
        if after is not None:
            north = jnp.where(row == 7, pltpu.roll(after, 7, 0), north)
        if before is not None:
            south = jnp.where(row == 0, pltpu.roll(before, 1, 0), south)
        return step(mid, north, south)

    def tile(ref, t):
        return ref[8 * t : 8 * t + 8, :]

    def keep(t, second):
        for g in range(4):
            for q in range(4):
                at = 512 * g + 128 * q
                x2b[q, 8 * t : 8 * t + 8, 128 * g : 128 * g + 128] = second[:, at : at + 128]

    def term(t, second):
        return tile(mb, t) + later * tile(xb, t) - 0.5 * second

    def send_prior(q, when):
        send(x2b.at[q], pb.at[q], e_send, e_recv.at[q], at_win(lax.rem(w + 1, 16)), when)

    def relay_prior():
        wait(rel, rel_recv)
        for q in (2, 3):
            send(rel.at[q - 2], pb.at[q], rel_send, e_recv.at[q], at_win(jnp.int32(8)))

    loads[0].wait()
    first = [tile(xb, t) for t in range(4)]
    for t in range(4):
        x1b[8 * t : 8 * t + 8, :] = advanced(
            first[t - 1] if t > 0 else None, first[t], first[t + 1] if t < 3 else None
        )
    loads[1].wait()
    for t in range(4):
        second = advanced(
            tile(x1b, t - 1) if t > 0 else None, tile(x1b, t), tile(x1b, t + 1) if t < 3 else None
        )
        if t in (1, 2):
            keep(t, second)
        a = term(t, second)
        for g in range(4):
            for s in range(2):
                a_out[16 * s + slot_of(t, g)] = a[:, 512 * g + 256 * s : 512 * g + 256 * s + 256]
    pl.semaphore_wait(barrier, 46)
    north_of, south_of = lax.rem(l + 1, 32), lax.rem(l + 31, 32)
    send(xb.at[24:32, :], halo.at[0], h_send.at[0], h_recv.at[0], at_lat(north_of), l < 31)
    send(xb.at[0:8, :], halo.at[1], h_send.at[1], h_recv.at[1], at_lat(south_of), l > 0)

    def send_a(s, some):
        for v, device in some:
            send(a_out.at[16 * s + v], a_in.at[s, w], a_send, a_recv.at[s], device, w < 15)

    send_a(0, windows)
    send_a(1, windows[:7])
    for s in range(2):
        a_in[s, w] = a_out[16 * s + w]

    @pl.when(l == 0)
    def _():
        halo[0] = jnp.zeros((8, 2048), F32)

    @pl.when(l == 31)
    def _():
        halo[1] = jnp.zeros((8, 2048), F32)

    @pl.when(w == 0)
    def _():
        pb[...] = jnp.zeros(pb.shape, F32)
        p_in[...] = jnp.zeros(p_in.shape, F32)
        ep_in[...] = jnp.zeros(ep_in.shape, F32)

    wait(halo.at[0], h_recv.at[0], l > 0)
    wait(halo.at[1], h_recv.at[1], l < 31)
    low, high = halo[0], halo[1]
    beyond_low = jnp.where(l > 0, advanced(None, low, tile(xb, 0)), 0.0)
    edge = advanced(low, tile(xb, 0), tile(xb, 1))
    x1b[0:8, :] = edge
    bottom = advanced(beyond_low, edge, tile(x1b, 1))
    beyond_high = jnp.where(l < 31, advanced(tile(xb, 3), high, None), 0.0)
    edge = advanced(tile(xb, 2), tile(xb, 3), high)
    x1b[24:32, :] = edge
    top = advanced(tile(x1b, 2), edge, beyond_high)
    keep(0, bottom)
    keep(3, top)
    outer = jnp.where(row < 4, term(0, bottom), term(3, top))
    packed = jnp.where((row8 < 2) | (row8 >= 6), outer[:, :1024], pltpu.roll(outer[:, 1024:], 4, 0))
    holder = lax.rem(y, 2) == xh
    for k in range(8):
        ea_out[k] = packed[:, 128 * k : 128 * k + 128]
    for off in AROUND:
        k = ahead(y, off)
        row_of = lax.rem(k, 2)
        v = row_of * 8 + k
        send(ea_out.at[k], ea_in.at[w], ea_send, ea_recv, (row_of, k, z, xl, core), jnp.logical_and(w < 15, w != v))
    send_a(1, windows[7:])
    ea_in[w] = ea_out[y]
    send_prior(0, w < 15)
    for q in (2, 3):
        send(x2b.at[q], rel.at[q - 2], e_send, rel_recv, at_win(jnp.int32(15)), w == 7)
    send_prior(1, w == 7)

    loads[2].wait()
    loads[3].wait()
    for t in range(4):
        rows = slice(8 * t, 8 * t + 8)
        for g in range(4):
            for q in range(4):
                at = slice(512 * g + 128 * q, 512 * g + 128 * q + 128)
                u = mb[rows, at] + later * xb[rows, at]
                lamb[rows, at] = u
                lb[rows, at] = (
                    kb[0, rows, at].astype(F32) * (ob[0, rows, at] - x1b[rows, at])
                    + kb[1, rows, at].astype(F32) * (ob[1, rows, at] - x2b[q, rows, 128 * g : 128 * g + 128])
                    + u
                )

    def piece(s):
        wait_either(w == 15, a_in.at[s, 0:15], a_in.at[s, 0:14], a_recv.at[s])
        total = jnp.zeros((8, 256), F32)
        for v in range(16):
            p_out[32 * s + v] = total[:, :128]
            p_out[32 * s + 16 + v] = total[:, 128:]
            if v < 15:
                total = total + a_in[s, v]
        for q in (2 * s, 2 * s + 1):
            for v, device in windows:
                send(p_out.at[16 * q + v], p_in.at[q, w], p_send, p_recv.at[q], device, v > 0)
            if q == 1:
                send_prior(q, jnp.logical_and(w < 15, w != 7))
        if s == 1:
            for q in (2, 3):
                send_prior(q, jnp.logical_and(w < 15, w != 7))
        for q in (2 * s, 2 * s + 1):
            p_in[q, w] = p_out[16 * q + w]

    piece(0)

    @pl.when(holder)
    def _():
        wait_either(w == 15, ea_in.at[0:15], ea_in.at[0:14], ea_recv)
        total = jnp.zeros((8, 128), F32)
        for v in range(16):
            ep_out[v] = total
            if v < 15:
                total = total + ea_in[v]
        for v, device in windows:
            send(ep_out.at[v], ep_in.at[y], ep_send, ep_recv, device, v > 0)
        ep_in[y] = ep_out[w]

    piece(1)
    pl.when(w == 15)(relay_prior)

    for load in loads[4:]:
        load.wait()
    lsf[...] = gathered(ls[...], 32, 32) * 2.0**-22
    lnf[...] = gathered(lo[...], 16, 128)
    save_scale = pltpu.make_async_copy(lnf, lon_scale, out_sem.at[0])
    save_scale.start()

    @pl.when(w > 0)
    def _():
        wait_either(holder, ep_in.at[0:7], ep_in.at[0:8], ep_recv)

    for q in range(4):
        wait(p_in.at[q, 0:15], p_recv.at[q], w > 0)
        wait(pb.at[q], e_recv.at[q], w > 0)
        for g in range(4):
            at = slice(512 * g + 128 * q, 512 * g + 128 * q + 128)
            outer = ep_in[4 * (g % 2) + q]
            if g >= 2:
                outer = pltpu.roll(outer, 4, 0)
            for t in range(4):
                rows = slice(8 * t, 8 * t + 8)
                prior = 0.5 * pb[q, rows, 128 * g : 128 * g + 128]
                lamb[rows, at] = lamb[rows, at] - prior
                earlier = p_in[q, slot_of(t, g)]
                if t == 0:
                    earlier = jnp.where(row1 < 2, outer, earlier)
                if t == 3:
                    earlier = jnp.where(row1 >= 6, outer, earlier)
                rb[32 * g + 8 * t : 32 * g + 8 * t + 8, :] = lb[rows, at] - prior - (earlier + prior) * inv
        tb[q] = rb[...].T
        for off in AROUND:
            to = ahead(z, off)
            when = None if off else (group != q)
            device = (xh, y, to, jnp.int32(q // 2), jnp.int32(q % 2))
            send(tb.at[q, pl.ds(pl.multiple_of(to * 16, 16), 16), :], zb.at[l], z_send, z_recv, device, when)
    here = pl.ds(pl.multiple_of(z * 16, 16), 16)
    zb[l] = tb[group, here, :]
    save = pltpu.make_async_copy(lamb, new_mult, out_sem.at[1])
    save.start()

    wait(zb.at[0:31], z_recv)

    def sink(j, h, value):
        ob2[j, 8 * h : 8 * h + 8, :] = value

    operator(
        lambda j, h: zb[j, 8 * h : 8 * h + 8, :], sink, 32, 16, rows_of(twb, 0, 32), rows_of(twb, 32, 32), lsf, uv, wfb, wbb
    )
    for m, device in bands:
        send(ob2.at[m], turned.at[group, here, :], y_send, y_recv, device)
    own = pltpu.make_async_copy(ob2.at[l], turned.at[group, here, :], out_sem.at[2])
    own.start()

    wait(halo.at[0], h_send.at[0], l < 31)
    wait(halo.at[1], h_send.at[1], l > 0)

    @pl.when(w < 15)
    def _():
        wait(a_out.at[0:30], a_send)
        wait(x2b, e_send)
        wait_either(holder, ea_out.at[0:7], ea_out.at[0:8], ea_send)

    wait_either(w == 0, p_out.at[0:60], p_out.at[0:56], p_send)

    @pl.when(holder)
    def _():
        wait_either(w == 0, ep_out.at[0:15], ep_out.at[0:14], ep_send)

    wait(rel, rel_send, w == 15)
    wait(zb.at[0:31], z_send)
    save_scale.wait()
    save.wait()
    own.wait()
    wait(ob2.at[0:31], y_send)
    wait(ob2.at[0:31], y_recv)


def longitude_kernel(
    state, lam, turned, lon_scale, tw, wf, wb,
    new_state, new_mult,
    xb, lamb, yb, lnf, twb, wfb, wbb, vb, uv, outb, in_sem, out_sem,
):
    loads = [
        pltpu.make_async_copy(src, dst, in_sem.at[i])
        for i, (src, dst) in enumerate(
            [(turned, yb), (tw, twb), (wf, wfb), (lon_scale, lnf), (wb, wbb), (state, xb), (lam, lamb)]
        )
    ]
    for load in loads:
        load.start()
    loads[0].wait()
    loads[1].wait()
    for q in range(4):
        flat = yb[q].T
        for g in range(4):
            vb[4 * g + q] = flat[32 * g : 32 * g + 32, :]
    for load in loads[2:5]:
        load.wait()
    save = pltpu.make_async_copy(lamb, new_mult, out_sem.at[4])
    results = [
        pltpu.make_async_copy(outb.at[8 * h : 8 * h + 8, :], new_state.at[8 * h : 8 * h + 8, :], out_sem.at[h]) for h in range(4)
    ]

    def sink(j, h, value):
        if (j, h) == (0, 0):
            loads[5].wait()
            loads[6].wait()
            save.start()
        rows, columns = slice(8 * h, 8 * h + 8), slice(128 * j, 128 * j + 128)
        outb[rows, columns] = xb[rows, columns] + value
        if j == 15:
            results[h].start()

    operator(lambda j, h: vb[j, 8 * h : 8 * h + 8, :], sink, 16, 32, rows_of(twb, 0, 16), rows_of(twb, 16, 16), lnf, uv, wfb, wbb)
    save.wait()
    for result in results:
        result.wait()


def per_device(state, multipliers, observations, obs_mask, speed, drift, kappa, lat_spectrum, lon_spectrum):
    band, nlon = state.shape[2:]
    (tw_lat, w_lat), (tw_lon, w_lon) = tables(32, 32), tables(16, 128)
    hbm = pl.BlockSpec(memory_space=pltpu.HBM)
    vmem = pltpu.VMEM
    dma = pltpu.SemaphoreType.DMA
    grid = jax.ShapeDtypeStruct((band, nlon), F32)
    field = vmem((32, 2048), F32)
    turned, lam, lon_scale = pl.pallas_call(
        exchange_kernel,
        out_shape=[jax.ShapeDtypeStruct((4, 128, 128), F32), grid, jax.ShapeDtypeStruct((16, 128), F32)],
        in_specs=[hbm] * 4 + [pl.BlockSpec(memory_space=pltpu.SMEM)] * 3 + [hbm] * 5,
        out_specs=[hbm] * 3,
        scratch_shapes=[
            field, field, vmem((2, 32, 2048), F32), vmem((2, 32, 2048), jnp.int32),
            vmem((1, 1024), F32), vmem((1, 2048), F32), vmem((64, 128), F32), vmem((256, 256), BF16), vmem((384, 256), BF16),
            vmem((2, 8, 2048), F32), field, vmem((4, 32, 512), F32), vmem((4, 32, 512), F32), field, field,
            vmem((32, 8, 256), F32), vmem((2, 16, 8, 256), F32), vmem((64, 8, 128), F32), vmem((4, 16, 8, 128), F32),
            vmem((8, 8, 128), F32), vmem((16, 8, 128), F32), vmem((16, 8, 128), F32), vmem((8, 8, 128), F32), vmem((2, 32, 512), F32),
            vmem((128, 128), F32), vmem((4, 128, 128), F32), vmem((32, 16, 128), F32), vmem((32, 16, 128), F32),
            vmem((512, 256), F32), vmem((32, 128), F32), vmem((16, 128), F32),
            dma((9,)), dma((3,)), dma((2,)), dma((2,)), dma, dma((2,)), dma, dma((4,)),
            dma, dma, dma, dma, dma, dma((4,)), dma, dma, dma, dma, dma, dma,
        ],
        compiler_params=pltpu.CompilerParams(collective_id=0, has_side_effects=True, vmem_limit_bytes=67043328),
        name="exchange",
    )(
        state[0, 0], multipliers[0, 0], observations[0, :, 0], obs_mask[0], speed, drift, kappa, lat_spectrum, lon_spectrum,
        jnp.asarray(tw_lat), *(jnp.asarray(part) for part in weights(w_lat)),
    )
    new_state, new_mult = pl.pallas_call(
        longitude_kernel,
        out_shape=[grid] * 2,
        in_specs=[hbm] * 7,
        out_specs=[hbm] * 2,
        scratch_shapes=[
            field, field, vmem((4, 128, 128), F32), vmem((16, 128), F32), vmem((32, 128), F32),
            vmem((256, 256), BF16), vmem((384, 256), BF16), vmem((16, 32, 128), F32), vmem((512, 256), F32), field,
            dma((7,)), dma((5,)),
        ],
        compiler_params=pltpu.CompilerParams(vmem_limit_bytes=67043328),
        name="longitudes",
    )(
        state[0, 0], lam, turned, lon_scale,
        jnp.asarray(tw_lon), *(jnp.asarray(part) for part in weights(w_lon)),
    )
    return new_state[None, None], new_mult[None, None]


def solution(mesh):
    finer = Mesh(mesh.devices.reshape(2, 8, 8, 2, 2), AXES)
    placed = (
        P(WIN, None, LAT, None),
        P(WIN, None, LAT, None),
        P(WIN, None, None, LAT, None),
        P(WIN, None, LAT, None),
        P(),
        P(),
        P(),
        P(),
        P(),
    )
    return jax.shard_map(
        per_device,
        mesh=finer,
        in_specs=placed,
        out_specs=(P(WIN, None, LAT, None), P(WIN, None, LAT, None)),
        check_vma=False,
    )
```
